128 devices in a mesh: grp: 4 (over y), gx: 8 (over x_hi, z), gy: 4 (over x_lo, core).
Axes of the slice: x: 4 (x_hi: 2, x_lo: 2; x = x_hi * 2 + x_lo), y: 4, z: 4, core: 2. Of those that a mesh axis runs over, the one named last changes fastest.
Arguments:
- terminal: float32 [4, 32, 64, 512], P(None, 'gx', 'gy', 'grp'), may hold values from -6 to 6
- diffusion: float32 [4], replicated, may hold values from 0.03 to 0.1
- velocity: float32 [32, 64, 512], P('gx', 'gy', 'grp'), may hold values from 0.02 to 0.3
- material: int32 [32, 64, 512], P('gx', 'gy', 'grp'), may hold values from 0 to 7
- rates: float32 [8, 8], replicated, may hold values from 0.005 to 0.04
- stoich: int32 [8, 4], replicated, may hold values from -1 to 1
- plan: int32 [8], replicated, may hold values from 0 to 15, as said below
- basis: bfloat16 [4, 32, 64, 512, 256], P('grp', 'gx', 'gy')
Outputs:
- coefficients: float32 [8, 256], replicated
- adjoint: float32 [4, 32, 64, 512], P(None, 'gx', 'gy', 'grp')
The draws below stay inside these ranges and needn't reach their ends.
Inputs may be any that keep to these rules, and one draw needn't show every extreme that they name: `plan`: 8 different step numbers in increasing order.
All inputs are finite; a program needn't handle non-finite values.
Results may differ from the reference program's by a relative error of at most 0.0045.
Values sent between devices are 32-bit elements; how exact they have to be, the bound alone decides.
A program may use at most 64 MiB of HBM per device.

```python
import math
import jax
import jax.numpy as jnp
from jax import lax

SPEC = 4
MODES = 256
REACT = 8
MATS = 8
STEPS = 16
SNAPS = 8
NX = 32
NY = 64
NZ = 512


def draw_plan(key, part):
    order = jax.random.permutation(jax.random.fold_in(key, 5), STEPS)
    return jnp.sort(order[:SNAPS]).astype(jnp.int32)


def draw_basis(key, part):
    total_rows = SPEC * NX * NY * NZ
    base = jax.random.fold_in(key, 11)
    share = jax.random.normal(jax.random.fold_in(base, 1), (MODES,), jnp.float32) * (2.0 / MODES) ** 0.5

    def make_block(index):
        noise_key = jax.random.fold_in(jax.random.fold_in(base, 2), index)
        common_key = jax.random.fold_in(jax.random.fold_in(base, 3), index)
        noise = jax.random.normal(noise_key, (NY * NZ, MODES), jnp.float32)
        common = jax.random.normal(common_key, (NY * NZ, 1), jnp.float32)
        return ((noise + common * share[None, :]) * total_rows ** (-0.5)).astype(jnp.bfloat16)
    return lax.map(make_block, jnp.arange(SPEC * NX)).reshape(SPEC, NX, NY, NZ, MODES)


def set_ends(result, key, least, top_value):
    index_at = [jax.random.randint(jax.random.fold_in(key, axis), (), 0, length) for axis, length in enumerate(result.shape)]
    main_axis = result.shape.index(max(result.shape))
    neighbour = index_at[:main_axis] + [(index_at[main_axis] + 1) % result.shape[main_axis]] + index_at[main_axis + 1:]
    return result.at[tuple(index_at)].set(least).at[tuple(neighbour)].set(top_value)


def levels(stream_key, extent, split, least, largest):
    level = 1.0
    for dim, shards_of in split:
        draws = jax.random.uniform(jax.random.fold_in(jax.random.fold_in(stream_key, 6), dim), (shards_of,), jnp.float32, least / len(split), largest / len(split))
        level = level * jnp.repeat(jnp.exp(draws), extent[dim] // shards_of).reshape((-1,) + (1,) * (len(extent) - 1 - dim))
    return level


def normal_values(key, shape, scale, most, shards=(), kind=jnp.bfloat16):
    drawn = scale * jax.random.normal(key, shape, jnp.float32)
    if shards:
        drawn = drawn * levels(key, shape, shards, -0.22, 0.18)
    return jnp.clip(drawn, -most, most).astype(kind)


def setup_inputs(seed: int = 0) -> dict:
    arg_keys = jax.random.split(jax.random.key(seed), 9)
    return {
        "terminal": normal_values(arg_keys[0], (SPEC, NX, NY, NZ), 1.0, 6.0, ((1, 8), (2, 4), (3, 4)), jnp.float32),
        "diffusion": jnp.clip(jnp.exp(jax.random.uniform(arg_keys[1], (SPEC,), jnp.float32, math.log(0.03), math.log(0.1))), 0.03, 0.1),
        "velocity": jnp.clip(0.02 + 0.28 * jax.random.uniform(arg_keys[2], (NX, NY, NZ), jnp.float32) ** levels(arg_keys[2], (NX, NY, NZ), ((0, 8), (1, 4), (2, 4)), -0.2, 0.2), 0.02, 0.3),
        "material": set_ends(jax.random.randint(arg_keys[3], (NX, NY, NZ), 0, MATS), jax.random.fold_in(arg_keys[3], 1), 0, MATS - 1).astype(jnp.int32),
        "rates": jnp.clip(jnp.exp(jax.random.uniform(arg_keys[4], (MATS, REACT), jnp.float32, math.log(0.005), math.log(0.04))), 0.005, 0.04),
        "stoich": set_ends(jax.random.randint(arg_keys[5], (REACT, SPEC), -1, 2), jax.random.fold_in(arg_keys[5], 1), -1, 1).astype(jnp.int32),
        "plan": draw_plan(jax.random.fold_in(arg_keys[8], 71), 0),
        "basis": draw_basis(jax.random.fold_in(arg_keys[8], 71), 0),
    }


def reaction_table(rates, stoich):
    react_count, spec = stoich.shape
    owner = jnp.arange(react_count) % spec
    pick = (owner[:, None] == jnp.arange(spec)[None, :]).astype(jnp.float32)
    return jnp.einsum("mr,ra,rs->mas", rates.astype(jnp.float32), pick, stoich.astype(jnp.float32), precision=lax.Precision.HIGHEST)


def advance(padded, diffusion, velocity, react):
    center = padded[:, 1:-1, 1:-1, 1:-1]
    ahead = padded[:, 2:, 1:-1, 1:-1]
    beside = ahead + padded[:, :-2, 1:-1, 1:-1]
    beside = beside + padded[:, 1:-1, 2:, 1:-1] + padded[:, 1:-1, :-2, 1:-1]
    beside = beside + padded[:, 1:-1, 1:-1, 2:] + padded[:, 1:-1, 1:-1, :-2]
    spec = center.shape[0]
    sources = []
    for first in range(spec):
        total = react[first * spec] * center[0]
        for second in range(1, spec):
            total = total + react[first * spec + second] * center[second]
        sources.append(total)
    source = jnp.stack(sources)
    return center + diffusion[:, None, None, None] * (beside - 6.0 * center) + velocity[None] * (ahead - center) + source


def reference(terminal, diffusion, velocity, material, rates, stoich, plan, basis):
    table = reaction_table(rates, stoich).reshape(MATS, SPEC * SPEC)
    react = jnp.moveaxis(table[material], -1, 0)

    def single(lam, index):
        padded = jnp.pad(lam, ((0, 0), (1, 1), (1, 1), (1, 1)))
        lam = advance(padded, diffusion, velocity, react)
        return lam, lam

    final, states = lax.scan(single, terminal, jnp.arange(STEPS))
    snaps = states[plan]
    blocks = SPEC * NX
    width = NY * NZ
    ubl = basis.reshape(blocks, width, MODES)
    abl = jnp.transpose(snaps.reshape(SNAPS, blocks, width), (1, 0, 2))

    def first_part(pair):
        upart, apart = pair
        return jnp.dot(apart.astype(jnp.bfloat16), upart, preferred_element_type=jnp.float32)

    first = jnp.sum(lax.map(first_part, (ubl, abl)), axis=0)
    first_low = first.astype(jnp.bfloat16)

    def second_part(pair):
        upart, apart = pair
        proj = lax.dot_general(first_low, upart, (((1,), (1,)), ((), ())), preferred_element_type=jnp.float32)
        rest = apart - proj
        return jnp.dot(rest.astype(jnp.bfloat16), upart, preferred_element_type=jnp.float32)

    second = jnp.sum(lax.map(second_part, (ubl, abl)), axis=0)
    return first + second, final
```

```python
import jax
import jax.numpy as jnp
from jax import lax
from jax.experimental import pallas as pl
from jax.experimental.pallas import tpu as pltpu
from jax.sharding import PartitionSpec as P

SPEC = 4
MATS = 8
STEPS = 16
ROUNDS = STEPS // 2
SNAPS = 8
MODES = 256
CX, CY, CZ = 4, 16, 128
ROWS = CX * CY
BASIS_ROWS = ROWS * 512
PART = BASIS_ROWS // ROUNDS
MESH = pl.DeviceIdType.MESH
F32 = jnp.float32
BF16 = jnp.bfloat16

FACES = [(-1, 0, 0), (1, 0, 0), (0, -1, 0), (0, 1, 0), (0, 0, -1), (0, 0, 1)]
XZ = [(a, 0, b) for a in (-1, 1) for b in (-1, 1)]
XY = [(a, b, 0) for a in (-1, 1) for b in (-1, 1)]
YZ = [(0, a, b) for a in (-1, 1) for b in (-1, 1)]
DIRS = FACES + XZ + XY + YZ
ORDER = [0, 1, 6, 7, 8, 9, 10, 11, 12, 13, 4, 5, 14, 15, 16, 17, 2, 3]


def kernel(
    terminal, diffusion, velocity, material, rates, stoich, plan, basis,
    coeff_out, adj_out,
    bv, st, fields, rx, ry, rz, pack, edge, cx, cy, cz, lam, mid,
    kc, vm, dm, rc, gram, got, proj, suma, sumb,
    basis_sem, hs, hr, cs, cr, as_, ar, ss, sr,
):
    g = lax.axis_index("grp")
    x = lax.axis_index("gx")
    y = lax.axis_index("gy")
    n_g, n_x, n_y = 4, 8, 4

    def has(d):
        cond = None
        for step, at, count in ((d[0], x, n_x), (d[1], y, n_y), (d[2], g, n_g)):
            if step == 0:
                continue
            term = at > 0 if step < 0 else at < count - 1
            cond = term if cond is None else jnp.logical_and(cond, term)
        return cond

    def minus(d):
        return tuple(-v for v in d)

    def dev(d):
        return (g + d[2], x + d[0], y + d[1])

    sub = lax.broadcasted_iota(jnp.int32, (8, CZ), 0)
    lane = lax.broadcasted_iota(jnp.int32, (8, CZ), 1)
    odd_lane = lax.rem(lane, 2) == 1
    odd_sub = lax.rem(sub, 2) == 1

    def low(cond, most):
        return jnp.where(cond, most, 0)

    def high(cond, least, size):
        return jnp.where(cond, least, size)

    def basis_copy(c):
        rows = pl.ds(c * PART, PART)
        return pltpu.make_async_copy(basis.at[rows, :], bv.at[rows, :], basis_sem.at[c])

    for c in range(ROUNDS):
        basis_copy(c).start()

    st[0] = terminal[...]
    fields[0] = velocity[...]
    fields[1] = material[...].astype(F32)
    lam[...] = jnp.zeros_like(lam)

    barrier = pltpu.get_barrier_semaphore()
    ga = g * n_y + y

    def group_a(o):
        q = lax.rem(ga + o, n_g * n_y)
        return q, (q // n_y, x, lax.rem(q, n_y))

    def group_b(o):
        q = lax.rem(x + o, n_x)
        return q, (g, q, y)

    count = jnp.int32(n_g * n_y - 1 + n_x - 1)
    for o in range(1, n_g * n_y):
        pl.semaphore_signal(barrier, inc=1, device_id=group_a(o)[1], device_id_type=MESH)
    for o in range(1, n_x):
        pl.semaphore_signal(barrier, inc=1, device_id=group_b(o)[1], device_id_type=MESH)
    for d in XZ + XY:
        cond = has(d)
        count = count + cond.astype(jnp.int32)

        @pl.when(cond)
        def _(d=d):
            pl.semaphore_signal(barrier, inc=1, device_id=dev(d), device_id_type=MESH)

    pl.semaphore_wait(barrier, count)

    def halo_copy(i, k, par):
        d = DIRS[i]
        n = 2 * k
        if i < 2:
            src = st.at[n, :, pl.ds(0 if i == 0 else 2, 2)]
            dst = rx.at[par, i]
        elif i < 4:
            src = st.at[n, :, :, pl.ds(0 if i == 2 else 8, 8), :]
            dst = ry.at[par, i - 2]
        elif i < 6:
            src = st.at[n]
            dst = rz.at[par, i - 4]
        else:
            if i < 10:
                which = (i - 6) // 2
            elif i < 14:
                which = 2 + (i - 10) // 2
            else:
                which = 4
            src = pack.at[par, which]
            dst = edge.at[par, i - 6]
        return pltpu.make_async_remote_copy(
            src_ref=src, dst_ref=dst, send_sem=hs.at[par, i], recv_sem=hr.at[par, i],
            device_id=dev(d), device_id_type=MESH,
        )

    def pack_edges(k, par):
        n = 2 * k
        for side in (0, 1):
            plane = 0 if side == 0 else CX - 1
            acc = jnp.zeros((8, CZ), F32)
            rows = jnp.zeros((8, CZ), F32)
            for s in range(SPEC):
                t0 = st[n, s, plane, 0:8, :]
                t1 = st[n, s, plane, 8:16, :]
                for t, v in ((0, t0), (1, t1)):
                    i = 2 * (s * 2 + t)
                    hit = jnp.logical_or(lane == i, lane == (i - 1) % CZ)
                    acc = jnp.where(hit, pltpu.roll(v, i, 1) if i else v, acc)
                i = 2 * s
                both = jnp.where(sub < 4, t0, t1)
                hit = jnp.logical_or(sub == i, sub == (i - 1) % 8)
                rows = jnp.where(hit, pltpu.roll(both, i, 0) if i else both, rows)
            pack[par, side] = acc
            pack[par, 2 + side] = rows
        acc = jnp.zeros((8, CZ), F32)
        for s in range(SPEC):
            for p in range(CX):
                i = 2 * (s * CX + p)
                v = jnp.where(sub < 4, st[n, s, p, 0:8, :], st[n, s, p, 8:16, :])
                hit = jnp.logical_or(lane == i, lane == (i - 1) % CZ)
                acc = jnp.where(hit, pltpu.roll(v, i, 1) if i else v, acc)
        pack[par, 4] = acc

    def start_halo(k, par):
        pack_edges(k, par)
        for i in ORDER:

            @pl.when(has(DIRS[i]))
            def _(i=i):
                halo_copy(i, k, par).start()

    def wait_halo(k, par):
        for i in ORDER:

            @pl.when(has(minus(DIRS[i])))
            def _(i=i):
                halo_copy(i, k, par).wait_recv()

    def wait_sent(k, par):
        for i in ORDER:

            @pl.when(has(DIRS[i]))
            def _(i=i):
                halo_copy(i, k, par).wait_send()

    xm, xp = has((-1, 0, 0)), has((1, 0, 0))
    ym, yp = has((0, -1, 0)), has((0, 1, 0))
    zm, zp = has((0, 0, -1)), has((0, 0, 1))
    y_from_p = sub < low(yp, 4)
    y_from_m = sub >= high(ym, 4, 8)
    lane_full = lax.broadcasted_iota(jnp.int32, (CY, CZ), 1)
    z_from_p = lane_full < low(zp, 64)
    z_from_m = lane_full >= high(zm, 64, CZ)

    def unpack(par):
        zero8 = jnp.zeros((8, CZ), F32)
        for s in range(SPEC):
            lam[s, 0:2, 0:16, 0:128] = jnp.where(xm, rx[par, 1, s], 0.0)
            lam[s, 6:8, 0:16, 0:128] = jnp.where(xp, rx[par, 0, s], 0.0)
            for p in range(CX):
                lam[s, 2 + p, 16:24, 0:128] = jnp.where(
                    y_from_p, ry[par, 0, s, p], jnp.where(y_from_m, ry[par, 1, s, p], zero8))
                lam[s, 2 + p, 0:16, 128:256] = jnp.where(
                    z_from_p, rz[par, 0, s, p], jnp.where(z_from_m, rz[par, 1, s, p], 0.0))

        def flag(a, b):
            return jnp.logical_and(a, b)

        for side, xh in ((1, xm), (0, xp)):
            base = side * 2
            m_m, m_p = edge[par, base + 1], edge[par, base]
            comb = jnp.where(
                jnp.logical_and(odd_lane, lane < low(flag(xh, zm), CZ)), m_m,
                jnp.where(
                    jnp.logical_and(jnp.logical_not(odd_lane), lane < low(flag(xh, zp), CZ)),
                    m_p, zero8))
            at = 1 if side == 1 else 6
            for s in range(SPEC):
                for t in range(2):
                    i = 2 * (s * 2 + t)
                    tile = pltpu.roll(comb, (CZ - i) % CZ, 1) if i else comb
                    lam[s, at, t * 8:(t + 1) * 8, 128:256] = tile
        for side, xh in ((1, xm), (0, xp)):
            base = 4 + side * 2
            m_m, m_p = edge[par, base + 1], edge[par, base]
            comb = jnp.where(
                jnp.logical_and(odd_sub, sub < low(flag(xh, ym), 8)), m_m,
                jnp.where(
                    jnp.logical_and(jnp.logical_not(odd_sub), sub < low(flag(xh, yp), 8)),
                    m_p, zero8))
            at = 1 if side == 1 else 6
            for s in range(SPEC):
                i = 2 * s
                tile = pltpu.roll(comb, (8 - i) % 8, 0) if i else comb
                lam[s, at, 16:24, 0:128] = tile
        even_lane = jnp.logical_not(odd_lane)
        hi_m = jnp.logical_and(odd_lane, sub >= high(flag(ym, zm), 4, 8))
        hi_p = jnp.logical_and(even_lane, sub >= high(flag(ym, zp), 4, 8))
        lo_m = jnp.logical_and(odd_lane, sub < low(flag(yp, zm), 4))
        lo_p = jnp.logical_and(even_lane, sub < low(flag(yp, zp), 4))
        comb = jnp.where(hi_m, edge[par, 11], zero8)
        comb = jnp.where(hi_p, edge[par, 10], comb)
        comb = jnp.where(lo_m, edge[par, 9], comb)
        comb = jnp.where(lo_p, edge[par, 8], comb)
        for s in range(SPEC):
            for p in range(CX):
                i = 2 * (s * CX + p)
                tile = pltpu.roll(comb, (CZ - i) % CZ, 1) if i else comb
                lam[s, 2 + p, 16:24, 128:256] = tile

    def coeff_copy(i):
        if i < 2:
            src = fields.at[:, pl.ds(0 if i == 0 else CX - 1, 1)]
            dst = cx.at[i]
        elif i < 4:
            src = fields.at[:, :, pl.ds(0 if i == 2 else 8, 8), :]
            dst = cy.at[i - 2]
        else:
            src = fields
            dst = cz.at[i - 4]
        return pltpu.make_async_remote_copy(
            src_ref=src, dst_ref=dst, send_sem=cs.at[i], recv_sem=cr.at[i],
            device_id=dev(DIRS[i]), device_id_type=MESH,
        )

    for i in range(6):

        @pl.when(has(DIRS[i]))
        def _(i=i):
            coeff_copy(i).start()

    def snap_copy(k, o):
        q = lax.rem(g + o, n_g)
        return pltpu.make_async_remote_copy(
            src_ref=st.at[pl.ds(2 * k + 1, 2), q],
            dst_ref=got.at[pl.ds(2 * k, 2), g],
            send_sem=as_.at[k, o - 1], recv_sem=ar.at[k, o - 1],
            device_id=(q, x, y), device_id_type=MESH,
        )

    gram[...] = jnp.zeros_like(gram)
    lam[:, 2:6, 0:16, 0:128] = terminal[...]

    def coefficients():
        sub24 = lax.broadcasted_iota(jnp.int32, (24, 256), 0)
        lane24 = lax.broadcasted_iota(jnp.int32, (24, 256), 1)
        for p in range(6):
            own = 1 <= p <= CX
            for r0, r1, l0, l1 in ((0, 16, 0, 128), (16, 24, 0, 128), (0, 16, 128, 256)):
                if not own and (r0, l0) != (0, 0):
                    continue
                vals = []
                for f in range(2):
                    if not own:
                        side, ok = (1, xm) if p == 0 else (0, xp)
                        v = jnp.where(ok, cx[side, f, 0], 0.0)
                    elif (r0, l0) == (0, 0):
                        v = fields[f, p - 1]
                    elif r0 == 16:
                        v = jnp.where(y_from_p, cy[0, f, p - 1],
                                      jnp.where(y_from_m, cy[1, f, p - 1], 0.0))
                    else:
                        v = jnp.where(z_from_p, cz[0, f, p - 1],
                                      jnp.where(z_from_m, cz[1, f, p - 1], 0.0))
                    vals.append(v)
                vel, mat = vals
                if not own:
                    ok = xm if p == 0 else xp
                    inside = jnp.where(ok, 1.0, 0.0) * jnp.ones((16, 128), F32)
                elif (r0, l0) == (0, 0):
                    inside = jnp.ones((16, 128), F32)
                elif r0 == 16:
                    inside = jnp.where(jnp.logical_or(y_from_p, y_from_m), 1.0, 0.0)
                else:
                    inside = jnp.where(jnp.logical_or(z_from_p, z_from_m), 1.0, 0.0)
                looked = []
                for r in range(8):
                    v = jnp.full(mat.shape, rates[0, r], F32)
                    for m in range(1, MATS):
                        v = jnp.where(mat == float(m), rates[m, r], v)
                    looked.append(v * inside)
                vel = vel * inside
                vm[p, r0:r1, l0:l1] = vel
                for a in range(SPEC):
                    dm[a, p, r0:r1, l0:l1] = inside * diffusion[a]
                    for b in range(SPEC):
                        v = (looked[a] * stoich[a, b].astype(F32)
                             + looked[a + 4] * stoich[a + 4, b].astype(F32))
                        if a == b:
                            kc[a, p, r0:r1, l0:l1] = (
                                inside * (1.0 - 6.0 * diffusion[a]) - vel + v)
                        else:
                            rc[a, b, p, r0:r1, l0:l1] = v

    def advance(cs_, s, p, tile, dn, up, ys, zs):
        r0, r1, l0, l1 = tile
        box = (p, slice(r0, r1), slice(l0, l1))
        total = dm[(s,) + box] * (((dn + up) + ys) + zs)
        total = total + kc[(s,) + box] * cs_[s]
        total = total + vm[box] * up
        for b in range(SPEC):
            if b != s:
                total = total + rc[(s, b) + box] * cs_[b]
        return total

    own_tile = (0, 16, 0, 128)

    def first_step():
        for p in range(6):
            full = [lam[s, p + 1] for s in range(SPEC)]
            for s in range(SPEC):
                c = full[s]
                ya = pltpu.roll(c, 1, 0) + pltpu.roll(c, 23, 0)
                za = pltpu.roll(c, 1, 1) + pltpu.roll(c, 255, 1)
                tiles = [own_tile]
                if 1 <= p <= CX:
                    tiles += [(16, 24, 0, 128), (0, 16, 128, 256)]
                for t in tiles:
                    r0, r1, l0, l1 = t
                    mid[s, p, r0:r1, l0:l1] = advance(
                        [v[r0:r1, l0:l1] for v in full], s, p, t,
                        lam[s, p, r0:r1, l0:l1], lam[s, p + 2, r0:r1, l0:l1],
                        ya[r0:r1, l0:l1], za[r0:r1, l0:l1])

    def second_step(n):
        for p in range(1, 1 + CX):
            own = [mid[s, p, 0:16, 0:128] for s in range(SPEC)]
            for s in range(SPEC):
                col = mid[s, p, :, 0:128]
                ya = (pltpu.roll(col, 1, 0) + pltpu.roll(col, 23, 0))[0:16]
                row = mid[s, p, 0:16, :]
                za = (pltpu.roll(row, 1, 1) + pltpu.roll(row, 255, 1))[:, 0:128]
                new = advance(own, s, p, own_tile, mid[s, p - 1, 0:16, 0:128],
                              mid[s, p + 1, 0:16, 0:128], ya, za)
                st[n + 1, s, p - 1] = own[s]
                st[n + 2, s, p - 1] = new
                lam[s, p + 1, 0:16, 0:128] = new

    mid[...] = jnp.zeros_like(mid)

    def gram_part(k):
        rows = 512

        def one(c, carry):
            at = pl.multiple_of(k * PART + c * rows, rows)
            block = bv[pl.ds(at, rows), :]
            gram[...] += lax.dot_general(
                block, block, (((0,), (0,)), ((), ())), preferred_element_type=F32)
            return carry

        lax.fori_loop(0, PART // rows, one, 0)

    start_halo(0, 0)
    for i in range(6):

        @pl.when(has(minus(DIRS[i])))
        def _(i=i):
            coeff_copy(i).wait_recv()

    coefficients()

    def round_(k, carry):
        par = lax.rem(k, 2)

        @pl.when(k > 0)
        def _():
            start_halo(k, par)
            for o in range(1, n_g):
                snap_copy(k - 1, o).start()

        basis_copy(k).wait()
        gram_part(k)
        wait_halo(k, par)
        unpack(par)
        first_step()
        second_step(2 * k)
        wait_sent(k, par)
        got[pl.ds(2 * k, 2), g] = st[pl.ds(2 * k + 1, 2), g]
        return carry

    lax.fori_loop(0, ROUNDS, round_, 0)
    for o in range(1, n_g):
        snap_copy(ROUNDS - 1, o).start()
    adj_out[...] = st[STEPS]
    for i in range(6):

        @pl.when(has(DIRS[i]))
        def _(i=i):
            coeff_copy(i).wait_send()

    def snap_wait(k, carry):
        for o in range(1, n_g):
            snap_copy(k, o).wait_recv()
        return carry

    lax.fori_loop(0, ROUNDS, snap_wait, 0)

    flat = got.reshape(STEPS * 4 * ROWS, CZ)
    proj[...] = jnp.zeros_like(proj)

    def project(c, carry):
        total = jnp.zeros((2 * STEPS, MODES), F32)
        for u in range(4):
            at = c * 4 + u
            vals = [flat[pl.ds(zq * ROWS + at, STEPS, stride=4 * ROWS), :] for zq in range(4)]
            a = jnp.concatenate(vals, axis=1)
            hi = a.astype(BF16)
            lo = (a - hi.astype(F32)).astype(BF16)
            both = jnp.concatenate([hi, lo], axis=0)
            rows = pl.ds(pl.multiple_of(at * 512, 512), 512)
            total += jnp.dot(both, bv[rows, :], preferred_element_type=F32)
        proj[...] += total
        return carry

    lax.fori_loop(0, ROWS // 4, project, 0)

    slot = lax.broadcasted_iota(jnp.int32, (SNAPS, MODES), 0)
    step_of = jnp.zeros((SNAPS, MODES), jnp.int32)
    for j in range(SNAPS):
        step_of = jnp.where(slot == j, plan[j], step_of)
    first = jnp.zeros((SNAPS, MODES), F32)
    rest = jnp.zeros((SNAPS, MODES), F32)
    for n in range(STEPS):
        hit = step_of == n
        first = jnp.where(hit, jnp.broadcast_to(proj[n:n + 1, :], first.shape), first)
        rest = jnp.where(
            hit, jnp.broadcast_to(proj[STEPS + n:STEPS + n + 1, :], first.shape), rest)

    def all_sum(value, turn):
        suma[turn, ga] = value

        def a_copy(o):
            q, where = group_a(o)
            return pltpu.make_async_remote_copy(
                src_ref=suma.at[turn, ga], dst_ref=suma.at[turn, ga],
                send_sem=ss.at[turn, 0, o], recv_sem=sr.at[turn, 0, o],
                device_id=where, device_id_type=MESH)

        def b_copy(o):
            q, where = group_b(o)
            return pltpu.make_async_remote_copy(
                src_ref=sumb.at[turn, x], dst_ref=sumb.at[turn, x],
                send_sem=ss.at[turn, 1, o], recv_sem=sr.at[turn, 1, o],
                device_id=where, device_id_type=MESH)

        for o in range(1, n_g * n_y):
            a_copy(o).start()
        for o in range(1, n_g * n_y):
            a_copy(o).wait_recv()
        total = suma[turn, 0]
        for q in range(1, n_g * n_y):
            total = total + suma[turn, q]
        sumb[turn, x] = total
        for o in range(1, n_x):
            b_copy(o).start()
        for o in range(1, n_x):
            b_copy(o).wait_recv()
        total = sumb[turn, 0]
        for q in range(1, n_x):
            total = total + sumb[turn, q]

        def finish():
            for o in range(1, n_g * n_y):
                a_copy(o).wait_send()
            for o in range(1, n_x):
                b_copy(o).wait_send()

        return total, finish

    total, finish_0 = all_sum(first, 0)
    low_first = total.astype(BF16)
    gm = gram[...]
    g1 = gm.astype(BF16)
    left = gm - g1.astype(F32)
    g2 = left.astype(BF16)
    g3 = (left - g2.astype(F32)).astype(BF16)
    back = jnp.dot(low_first, g1, preferred_element_type=F32)
    back += jnp.dot(low_first, g2, preferred_element_type=F32)
    back += jnp.dot(low_first, g3, preferred_element_type=F32)
    second = (first - back) + rest
    more, finish_1 = all_sum(second, 1)
    coeff_out[...] = total + more
    finish_0()
    finish_1()

    def snap_sent(k, carry):
        for o in range(1, n_g):
            snap_copy(k, o).wait_send()
        return carry

    lax.fori_loop(0, ROUNDS, snap_sent, 0)


def body(terminal, diffusion, velocity, material, rates, stoich, plan, basis):
    vmem = pl.BlockSpec(memory_space=pltpu.VMEM)
    smem = pl.BlockSpec(memory_space=pltpu.SMEM)
    dma = pltpu.SemaphoreType.DMA
    v = pltpu.VMEM
    return pl.pallas_call(
        kernel,
        out_shape=(
            jax.ShapeDtypeStruct((SNAPS, MODES), F32),
            jax.ShapeDtypeStruct((SPEC, CX, CY, CZ), F32),
        ),
        in_specs=[vmem, smem, vmem, vmem, smem, smem, smem, pl.BlockSpec(memory_space=pl.ANY)],
        out_specs=(vmem, vmem),
        scratch_shapes=[
            v((BASIS_ROWS, MODES), BF16),
            v((STEPS + 1, SPEC, CX, CY, CZ), F32),
            v((2, CX, CY, CZ), F32),
            v((2, 2, SPEC, 2, CY, CZ), F32),
            v((2, 2, SPEC, CX, 8, CZ), F32),
            v((2, 2, SPEC, CX, CY, CZ), F32),
            v((2, 5, 8, CZ), F32),
            v((2, 12, 8, CZ), F32),
            v((2, 2, 1, CY, CZ), F32),
            v((2, 2, CX, 8, CZ), F32),
            v((2, 2, CX, CY, CZ), F32),
            v((SPEC, 8, 24, 256), F32),
            v((SPEC, 6, 24, 256), F32),
            v((SPEC, 6, 24, 256), F32),
            v((6, 24, 256), F32),
            v((SPEC, 6, 24, 256), F32),
            v((SPEC, SPEC, 6, 24, 256), F32),
            v((MODES, MODES), F32),
            v((STEPS, 4, CX, CY, CZ), F32),
            v((2 * STEPS, MODES), F32),
            v((2, 16, SNAPS, MODES), F32),
            v((2, 8, SNAPS, MODES), F32),
            dma((ROUNDS,)),
            dma((2, 18)),
            dma((2, 18)),
            dma((6,)),
            dma((6,)),
            dma((ROUNDS, 3)),
            dma((ROUNDS, 3)),
            dma((2, 2, 16)),
            dma((2, 2, 16)),
        ],
        compiler_params=pltpu.CompilerParams(
            collective_id=0, has_side_effects=True, vmem_limit_bytes=60 * 1024 * 1024
        ),
    )(
        terminal, diffusion, velocity, material, rates, stoich, plan,
        basis.reshape(BASIS_ROWS, MODES),
    )


def solution(mesh):
    return jax.shard_map(
        body,
        mesh=mesh,
        in_specs=(
            P(None, "gx", "gy", "grp"),
            P(),
            P("gx", "gy", "grp"),
            P("gx", "gy", "grp"),
            P(),
            P(),
            P(),
            P("grp", "gx", "gy", None, None),
        ),
        out_specs=(P(), P(None, "gx", "gy", "grp")),
        check_vma=False,
    )
```

```python
import jax
import jax.numpy as jnp
from jax import lax
from jax.experimental import pallas as pl
from jax.experimental.pallas import tpu as pltpu
from jax.sharding import PartitionSpec as P

SPEC = 4
MATS = 8
STEPS = 16
ROUNDS = STEPS // 2
SNAPS = 8
MODES = 256
CX, CY, CZ = 4, 16, 128
ROWS = CX * CY
BASIS_ROWS = ROWS * 512
PART = BASIS_ROWS // ROUNDS
MESH = pl.DeviceIdType.MESH
F32 = jnp.float32
BF16 = jnp.bfloat16

FACES = [(-1, 0, 0), (1, 0, 0), (0, -1, 0), (0, 1, 0), (0, 0, -1), (0, 0, 1)]
XZ = [(a, 0, b) for a in (-1, 1) for b in (-1, 1)]
XY = [(a, b, 0) for a in (-1, 1) for b in (-1, 1)]
YZ = [(0, a, b) for a in (-1, 1) for b in (-1, 1)]
DIRS = FACES + XZ + XY + YZ
ORDER = [0, 1, 6, 7, 8, 9, 10, 11, 12, 13, 4, 5, 14, 15, 16, 17, 2, 3]


def kernel(
    terminal, diffusion, velocity, material, rates, stoich, plan, basis,
    coeff_out, adj_out,
    bv, st, fields, rx, ry, rz, pack, edge, cx, cy, cz, lam, mid,
    kc, vm, dm, rc, gram, got, proj, suma, sumb, gparts, gsums, gfull,
    basis_sem, hs, hr, cs, cr, as_, ar, ss, sr, gs, gr,
):
    g = lax.axis_index("grp")
    x = lax.axis_index("gx")
    y = lax.axis_index("gy")
    n_g, n_x, n_y = 4, 8, 4

    def has(d):
        cond = None
        for step, at, count in ((d[0], x, n_x), (d[1], y, n_y), (d[2], g, n_g)):
            if step == 0:
                continue
            term = at > 0 if step < 0 else at < count - 1
            cond = term if cond is None else jnp.logical_and(cond, term)
        return cond

    def minus(d):
        return tuple(-v for v in d)

    def dev(d):
        return (g + d[2], x + d[0], y + d[1])

    sub = lax.broadcasted_iota(jnp.int32, (8, CZ), 0)
    lane = lax.broadcasted_iota(jnp.int32, (8, CZ), 1)
    odd_lane = lax.rem(lane, 2) == 1
    odd_sub = lax.rem(sub, 2) == 1

    def low(cond, most):
        return jnp.where(cond, most, 0)

    def high(cond, least, size):
        return jnp.where(cond, least, size)

    def basis_copy(c):
        rows = pl.ds(c * PART, PART)
        return pltpu.make_async_copy(basis.at[rows, :], bv.at[rows, :], basis_sem.at[c])

    for c in range(ROUNDS):
        basis_copy(c).start()

    st[0] = terminal[...]
    fields[0] = velocity[...]
    fields[1] = material[...].astype(F32)
    lam[...] = jnp.zeros_like(lam)

    barrier = pltpu.get_barrier_semaphore()
    ga = g * n_y + y

    def group_a(o):
        q = lax.rem(ga + o, n_g * n_y)
        return q, (q // n_y, x, lax.rem(q, n_y))

    def group_b(o):
        q = lax.rem(x + o, n_x)
        return q, (g, q, y)

    count = jnp.int32(n_g * n_y - 1 + n_x - 1)
    for o in range(1, n_g * n_y):
        pl.semaphore_signal(barrier, inc=1, device_id=group_a(o)[1], device_id_type=MESH)
    for o in range(1, n_x):
        pl.semaphore_signal(barrier, inc=1, device_id=group_b(o)[1], device_id_type=MESH)
    for d in XZ + XY:
        cond = has(d)
        count = count + cond.astype(jnp.int32)

        @pl.when(cond)
        def _(d=d):
            pl.semaphore_signal(barrier, inc=1, device_id=dev(d), device_id_type=MESH)

    pl.semaphore_wait(barrier, count)

    def halo_copy(i, k, par):
        d = DIRS[i]
        n = 2 * k
        if i < 2:
            src = st.at[n, :, pl.ds(0 if i == 0 else 2, 2)]
            dst = rx.at[par, i]
        elif i < 4:
            src = st.at[n, :, :, pl.ds(0 if i == 2 else 8, 8), :]
            dst = ry.at[par, i - 2]
        elif i < 6:
            src = pack.at[par, 5]
            dst = rz.at[par, i - 4]
        else:
            if i < 10:
                which = (i - 6) // 2
            elif i < 14:
                which = 2 + (i - 10) // 2
            else:
                which = 4
            src = pack.at[par, which]
            dst = edge.at[par, i - 6]
        return pltpu.make_async_remote_copy(
            src_ref=src, dst_ref=dst, send_sem=hs.at[par, i], recv_sem=hr.at[par, i],
            device_id=dev(d), device_id_type=MESH,
        )

    def pack_edges(k, par):
        n = 2 * k
        for side in (0, 1):
            plane = 0 if side == 0 else CX - 1
            acc = jnp.zeros((8, CZ), F32)
            rows = jnp.zeros((8, CZ), F32)
            for s in range(SPEC):
                t0 = st[n, s, plane, 0:8, :]
                t1 = st[n, s, plane, 8:16, :]
                for t, v in ((0, t0), (1, t1)):
                    i = 2 * (s * 2 + t)
                    hit = jnp.logical_or(lane == i, lane == (i - 1) % CZ)
                    acc = jnp.where(hit, pltpu.roll(v, i, 1) if i else v, acc)
                i = 2 * s
                both = jnp.where(sub < 4, t0, t1)
                hit = jnp.logical_or(sub == i, sub == (i - 1) % 8)
                rows = jnp.where(hit, pltpu.roll(both, i, 0) if i else both, rows)
            pack[par, side] = acc
            pack[par, 2 + side] = rows
        acc = jnp.zeros((8, CZ), F32)
        for s in range(SPEC):
            for p in range(CX):
                i = 2 * (s * CX + p)
                v = jnp.where(sub < 4, st[n, s, p, 0:8, :], st[n, s, p, 8:16, :])
                hit = jnp.logical_or(lane == i, lane == (i - 1) % CZ)
                acc = jnp.where(hit, pltpu.roll(v, i, 1) if i else v, acc)
        pack[par, 4] = acc
        acc = jnp.zeros((8, CZ), F32)
        for s in range(SPEC):
            for p in range(CX):
                for t in range(2):
                    i = 4 * ((s * CX + p) * 2 + t)
                    v = st[n, s, p, t * 8:(t + 1) * 8, :]
                    place = lax.rem(lane + (CZ + 2 - i), CZ)
                    acc = jnp.where(place < 4, pltpu.roll(v, i, 1) if i else v, acc)
        pack[par, 5] = acc

    def start_halo(k, par):
        pack_edges(k, par)
        for i in ORDER:

            @pl.when(has(DIRS[i]))
            def _(i=i):
                halo_copy(i, k, par).start()

    def wait_halo(k, par):
        for i in ORDER:

            @pl.when(has(minus(DIRS[i])))
            def _(i=i):
                halo_copy(i, k, par).wait_recv()

    def wait_sent(k, par):
        for i in ORDER:

            @pl.when(has(DIRS[i]))
            def _(i=i):
                halo_copy(i, k, par).wait_send()

    xm, xp = has((-1, 0, 0)), has((1, 0, 0))
    ym, yp = has((0, -1, 0)), has((0, 1, 0))
    zm, zp = has((0, 0, -1)), has((0, 0, 1))
    y_from_p = sub < low(yp, 4)
    y_from_m = sub >= high(ym, 4, 8)
    lane_full = lax.broadcasted_iota(jnp.int32, (CY, CZ), 1)
    z_from_p = lane_full < low(zp, 64)
    z_from_m = lane_full >= high(zm, 64, CZ)

    def unpack(par):
        zero8 = jnp.zeros((8, CZ), F32)
        far = lax.rem(lane, 4) >= 2
        comb = jnp.where(
            jnp.logical_and(far, lane < low(zm, CZ)), rz[par, 1],
            jnp.where(
                jnp.logical_and(jnp.logical_not(far), lane < low(zp, CZ)), rz[par, 0], zero8))
        for s in range(SPEC):
            for p in range(CX):
                for t in range(2):
                    i = 4 * ((s * CX + p) * 2 + t)
                    tile = pltpu.roll(comb, (CZ - i) % CZ, 1) if i else comb
                    lam[s, 2 + p, t * 8:(t + 1) * 8, 128:256] = tile
        for s in range(SPEC):
            lam[s, 0:2, 0:16, 0:128] = jnp.where(xm, rx[par, 1, s], 0.0)
            lam[s, 6:8, 0:16, 0:128] = jnp.where(xp, rx[par, 0, s], 0.0)
            for p in range(CX):
                lam[s, 2 + p, 16:24, 0:128] = jnp.where(
                    y_from_p, ry[par, 0, s, p], jnp.where(y_from_m, ry[par, 1, s, p], zero8))

        def flag(a, b):
            return jnp.logical_and(a, b)

        for side, xh in ((1, xm), (0, xp)):
            base = side * 2
            m_m, m_p = edge[par, base + 1], edge[par, base]
            comb = jnp.where(
                jnp.logical_and(odd_lane, lane < low(flag(xh, zm), CZ)), m_m,
                jnp.where(
                    jnp.logical_and(jnp.logical_not(odd_lane), lane < low(flag(xh, zp), CZ)),
                    m_p, zero8))
            at = 1 if side == 1 else 6
            for s in range(SPEC):
                for t in range(2):
                    i = 2 * (s * 2 + t)
                    tile = pltpu.roll(comb, (CZ - i) % CZ, 1) if i else comb
                    lam[s, at, t * 8:(t + 1) * 8, 128:256] = tile
        for side, xh in ((1, xm), (0, xp)):
            base = 4 + side * 2
            m_m, m_p = edge[par, base + 1], edge[par, base]
            comb = jnp.where(
                jnp.logical_and(odd_sub, sub < low(flag(xh, ym), 8)), m_m,
                jnp.where(
                    jnp.logical_and(jnp.logical_not(odd_sub), sub < low(flag(xh, yp), 8)),
                    m_p, zero8))
            at = 1 if side == 1 else 6
            for s in range(SPEC):
                i = 2 * s
                tile = pltpu.roll(comb, (8 - i) % 8, 0) if i else comb
                lam[s, at, 16:24, 0:128] = tile
        even_lane = jnp.logical_not(odd_lane)
        hi_m = jnp.logical_and(odd_lane, sub >= high(flag(ym, zm), 4, 8))
        hi_p = jnp.logical_and(even_lane, sub >= high(flag(ym, zp), 4, 8))
        lo_m = jnp.logical_and(odd_lane, sub < low(flag(yp, zm), 4))
        lo_p = jnp.logical_and(even_lane, sub < low(flag(yp, zp), 4))
        comb = jnp.where(hi_m, edge[par, 11], zero8)
        comb = jnp.where(hi_p, edge[par, 10], comb)
        comb = jnp.where(lo_m, edge[par, 9], comb)
        comb = jnp.where(lo_p, edge[par, 8], comb)
        for s in range(SPEC):
            for p in range(CX):
                i = 2 * (s * CX + p)
                tile = pltpu.roll(comb, (CZ - i) % CZ, 1) if i else comb
                lam[s, 2 + p, 16:24, 128:256] = tile

    def coeff_copy(i):
        if i < 2:
            src = fields.at[:, pl.ds(0 if i == 0 else CX - 1, 1)]
            dst = cx.at[i]
        elif i < 4:
            src = fields.at[:, :, pl.ds(0 if i == 2 else 8, 8), :]
            dst = cy.at[i - 2]
        else:
            src = fields
            dst = cz.at[i - 4]
        return pltpu.make_async_remote_copy(
            src_ref=src, dst_ref=dst, send_sem=cs.at[i], recv_sem=cr.at[i],
            device_id=dev(DIRS[i]), device_id_type=MESH,
        )

    for i in range(6):

        @pl.when(has(DIRS[i]))
        def _(i=i):
            coeff_copy(i).start()

    def snap_copy(k, o):
        q = lax.rem(g + o, n_g)
        return pltpu.make_async_remote_copy(
            src_ref=st.at[pl.ds(2 * k + 1, 2), q],
            dst_ref=got.at[pl.ds(2 * k, 2), g],
            send_sem=as_.at[k, o - 1], recv_sem=ar.at[k, o - 1],
            device_id=(q, x, y), device_id_type=MESH,
        )

    gram[...] = jnp.zeros_like(gram)
    lam[:, 2:6, 0:16, 0:128] = terminal[...]

    def coefficients():
        sub24 = lax.broadcasted_iota(jnp.int32, (24, 256), 0)
        lane24 = lax.broadcasted_iota(jnp.int32, (24, 256), 1)
        for p in range(6):
            own = 1 <= p <= CX
            for r0, r1, l0, l1 in ((0, 16, 0, 128), (16, 24, 0, 128), (0, 16, 128, 256)):
                if not own and (r0, l0) != (0, 0):
                    continue
                vals = []
                for f in range(2):
                    if not own:
                        side, ok = (1, xm) if p == 0 else (0, xp)
                        v = jnp.where(ok, cx[side, f, 0], 0.0)
                    elif (r0, l0) == (0, 0):
                        v = fields[f, p - 1]
                    elif r0 == 16:
                        v = jnp.where(y_from_p, cy[0, f, p - 1],
                                      jnp.where(y_from_m, cy[1, f, p - 1], 0.0))
                    else:
                        v = jnp.where(z_from_p, cz[0, f, p - 1],
                                      jnp.where(z_from_m, cz[1, f, p - 1], 0.0))
                    vals.append(v)
                vel, mat = vals
                if not own:
                    ok = xm if p == 0 else xp
                    inside = jnp.where(ok, 1.0, 0.0) * jnp.ones((16, 128), F32)
                elif (r0, l0) == (0, 0):
                    inside = jnp.ones((16, 128), F32)
                elif r0 == 16:
                    inside = jnp.where(jnp.logical_or(y_from_p, y_from_m), 1.0, 0.0)
                else:
                    inside = jnp.where(jnp.logical_or(z_from_p, z_from_m), 1.0, 0.0)
                looked = []
                for r in range(8):
                    v = jnp.full(mat.shape, rates[0, r], F32)
                    for m in range(1, MATS):
                        v = jnp.where(mat == float(m), rates[m, r], v)
                    looked.append(v * inside)
                vel = vel * inside
                vm[p, r0:r1, l0:l1] = vel
                for a in range(SPEC):
                    dm[a, p, r0:r1, l0:l1] = inside * diffusion[a]
                    for b in range(SPEC):
                        v = (looked[a] * stoich[b, a].astype(F32)
                             + looked[a + 4] * stoich[b, a + 4].astype(F32))
                        if a == b:
                            kc[a, p, r0:r1, l0:l1] = (
                                inside * (1.0 - 6.0 * diffusion[a]) - vel + v)
                        else:
                            rc[a, b, p, r0:r1, l0:l1] = v

    def advance(cs_, s, p, tile, dn, up, ys, zs):
        r0, r1, l0, l1 = tile
        box = (p, slice(r0, r1), slice(l0, l1))
        total = dm[(s,) + box] * (((dn + up) + ys) + zs)
        total = total + kc[(s,) + box] * cs_[s]
        total = total + vm[box] * up
        for b in range(SPEC):
            if b != s:
                total = total + rc[(s, b) + box] * cs_[b]
        return total

    own_tile = (0, 16, 0, 128)

    def first_step():
        for p in range(6):
            full = [lam[s, p + 1] for s in range(SPEC)]
            for s in range(SPEC):
                c = full[s]
                ya = pltpu.roll(c, 1, 0) + pltpu.roll(c, 23, 0)
                za = pltpu.roll(c, 1, 1) + pltpu.roll(c, 255, 1)
                tiles = [own_tile]
                if 1 <= p <= CX:
                    tiles += [(16, 24, 0, 128), (0, 16, 128, 256)]
                for t in tiles:
                    r0, r1, l0, l1 = t
                    mid[s, p, r0:r1, l0:l1] = advance(
                        [v[r0:r1, l0:l1] for v in full], s, p, t,
                        lam[s, p, r0:r1, l0:l1], lam[s, p + 2, r0:r1, l0:l1],
                        ya[r0:r1, l0:l1], za[r0:r1, l0:l1])

    def second_step(n):
        for p in range(1, 1 + CX):
            own = [mid[s, p, 0:16, 0:128] for s in range(SPEC)]
            for s in range(SPEC):
                col = mid[s, p, :, 0:128]
                ya = (pltpu.roll(col, 1, 0) + pltpu.roll(col, 23, 0))[0:16]
                row = mid[s, p, 0:16, :]
                za = (pltpu.roll(row, 1, 1) + pltpu.roll(row, 255, 1))[:, 0:128]
                new = advance(own, s, p, own_tile, mid[s, p - 1, 0:16, 0:128],
                              mid[s, p + 1, 0:16, 0:128], ya, za)
                st[n + 1, s, p - 1] = own[s]
                st[n + 2, s, p - 1] = new
                lam[s, p + 1, 0:16, 0:128] = new

    mid[...] = jnp.zeros_like(mid)

    def gram_part(k):
        rows = 512

        def one(c, carry):
            at = pl.multiple_of(k * 2 * PART + c * rows, rows)
            block = bv[pl.ds(at, rows), :]
            gram[...] += lax.dot_general(
                block, block, (((0,), (0,)), ((), ())), preferred_element_type=F32)
            return carry

        lax.fori_loop(0, 2 * PART // rows, one, 0)

    slab = MODES // (n_g * n_y)

    def slab_of(q):
        return pl.ds(pl.multiple_of(q * slab, slab), slab)

    def gram_a(o):
        q, where = group_a(o)
        return pltpu.make_async_remote_copy(
            src_ref=gram.at[slab_of(q), :], dst_ref=gparts.at[ga],
            send_sem=gs.at[0, o], recv_sem=gr.at[0, o], device_id=where, device_id_type=MESH)

    def gram_b(o):
        q, where = group_b(o)
        return pltpu.make_async_remote_copy(
            src_ref=gsums.at[x], dst_ref=gsums.at[x],
            send_sem=gs.at[1, o], recv_sem=gr.at[1, o], device_id=where, device_id_type=MESH)

    def gram_c(o):
        q, where = group_a(o)
        return pltpu.make_async_remote_copy(
            src_ref=gfull.at[slab_of(ga), :], dst_ref=gfull.at[slab_of(ga), :],
            send_sem=gs.at[2, o], recv_sem=gr.at[2, o], device_id=where, device_id_type=MESH)

    def gram_start():
        gparts[ga] = gram[slab_of(ga), :]
        for o in range(1, n_g * n_y):
            gram_a(o).start()

    def gram_middle():
        for o in range(1, n_g * n_y):
            gram_a(o).wait_recv()
        total = gparts[0]
        for q in range(1, n_g * n_y):
            total = total + gparts[q]
        gsums[x] = total
        for o in range(1, n_x):
            gram_b(o).start()

    def gram_last():
        for o in range(1, n_x):
            gram_b(o).wait_recv()
        total = gsums[0]
        for q in range(1, n_x):
            total = total + gsums[q]
        gfull[slab_of(ga), :] = total
        for o in range(1, n_g * n_y):
            gram_c(o).start()

    start_halo(0, 0)
    for i in range(6):

        @pl.when(has(minus(DIRS[i])))
        def _(i=i):
            coeff_copy(i).wait_recv()

    coefficients()

    def round_(k, carry):
        par = lax.rem(k, 2)

        @pl.when(k > 0)
        def _():
            start_halo(k, par)
            for o in range(1, n_g):
                snap_copy(k - 1, o).start()

        @pl.when(k < ROUNDS // 2)
        def _():
            basis_copy(2 * k).wait()
            basis_copy(2 * k + 1).wait()
            gram_part(k)

        @pl.when(k == ROUNDS // 2)
        def _():
            gram_start()

        @pl.when(k == ROUNDS // 2 + 1)
        def _():
            gram_middle()

        @pl.when(k == ROUNDS // 2 + 2)
        def _():
            gram_last()

        wait_halo(k, par)
        unpack(par)
        first_step()
        second_step(2 * k)
        wait_sent(k, par)
        got[pl.ds(2 * k, 2), g] = st[pl.ds(2 * k + 1, 2), g]
        return carry

    lax.fori_loop(0, ROUNDS, round_, 0)
    for o in range(1, n_g):
        snap_copy(ROUNDS - 1, o).start()
    adj_out[...] = st[STEPS]
    for i in range(6):

        @pl.when(has(DIRS[i]))
        def _(i=i):
            coeff_copy(i).wait_send()

    flat = got.reshape(STEPS * 4 * ROWS, CZ)
    proj[...] = jnp.zeros_like(proj)
    unroll = 8

    def project(zq):
        def one(c, carry):
            vals, blocks = [], []
            for u in range(unroll):
                at = c * unroll + u
                vals.append(flat[pl.ds(zq * ROWS + at, STEPS, stride=4 * ROWS), :])
                blocks.append(
                    bv[pl.ds(pl.multiple_of(at * 512 + zq * CZ, CZ), CZ), :])
            a = jnp.concatenate(vals, axis=1)
            hi = a.astype(BF16)
            lo = (a - hi.astype(F32)).astype(BF16)
            both = jnp.concatenate([hi, lo], axis=0)
            proj[...] += jnp.dot(
                both, jnp.concatenate(blocks, axis=0), preferred_element_type=F32)
            return carry

        lax.fori_loop(0, ROWS // unroll, one, 0)

    project(g)
    for o in (1, 3, 2):
        def snap_wait(k, carry, o=o):
            snap_copy(k, o).wait_recv()
            return carry

        lax.fori_loop(0, ROUNDS, snap_wait, 0)
        project(lax.rem(g + n_g - o, n_g))

    slot = lax.broadcasted_iota(jnp.int32, (SNAPS, MODES), 0)
    step_of = jnp.zeros((SNAPS, MODES), jnp.int32)
    for j in range(SNAPS):
        step_of = jnp.where(slot == j, plan[j], step_of)
    first = jnp.zeros((SNAPS, MODES), F32)
    for n in range(STEPS):
        row = proj[n:n + 1, :] + proj[STEPS + n:STEPS + n + 1, :]
        first = jnp.where(step_of == n, jnp.broadcast_to(row, first.shape), first)

    def all_sum(value):
        suma[ga] = value

        def a_copy(o):
            q, where = group_a(o)
            return pltpu.make_async_remote_copy(
                src_ref=suma.at[ga], dst_ref=suma.at[ga],
                send_sem=ss.at[0, o], recv_sem=sr.at[0, o],
                device_id=where, device_id_type=MESH)

        def b_copy(o):
            q, where = group_b(o)
            return pltpu.make_async_remote_copy(
                src_ref=sumb.at[x], dst_ref=sumb.at[x],
                send_sem=ss.at[1, o], recv_sem=sr.at[1, o],
                device_id=where, device_id_type=MESH)

        for o in range(1, n_g * n_y):
            a_copy(o).start()
        for o in range(1, n_g * n_y):
            a_copy(o).wait_recv()
        total = suma[0]
        for q in range(1, n_g * n_y):
            total = total + suma[q]
        sumb[x] = total
        for o in range(1, n_x):
            b_copy(o).start()
        for o in range(1, n_x):
            b_copy(o).wait_recv()
        total = sumb[0]
        for q in range(1, n_x):
            total = total + sumb[q]

        def finish():
            for o in range(1, n_g * n_y):
                a_copy(o).wait_send()
            for o in range(1, n_x):
                b_copy(o).wait_send()

        return total, finish

    total, finish = all_sum(first)
    low_first = total.astype(BF16)
    for o in range(1, n_g * n_y):
        gram_c(o).wait_recv()
    gm = gfull[...]
    g1 = gm.astype(BF16)
    left = gm - g1.astype(F32)
    g2 = left.astype(BF16)
    g3 = (left - g2.astype(F32)).astype(BF16)
    back = jnp.dot(low_first, g1, preferred_element_type=F32)
    back += jnp.dot(low_first, g2, preferred_element_type=F32)
    back += jnp.dot(low_first, g3, preferred_element_type=F32)
    coeff_out[...] = total + (total - back)
    finish()
    for o in range(1, n_g * n_y):
        gram_a(o).wait_send()
        gram_c(o).wait_send()
    for o in range(1, n_x):
        gram_b(o).wait_send()

    def snap_sent(k, carry):
        for o in range(1, n_g):
            snap_copy(k, o).wait_send()
        return carry

    lax.fori_loop(0, ROUNDS, snap_sent, 0)


def body(terminal, diffusion, velocity, material, rates, stoich, plan, basis):
    vmem = pl.BlockSpec(memory_space=pltpu.VMEM)
    smem = pl.BlockSpec(memory_space=pltpu.SMEM)
    dma = pltpu.SemaphoreType.DMA
    v = pltpu.VMEM
    return pl.pallas_call(
        kernel,
        out_shape=(
            jax.ShapeDtypeStruct((SNAPS, MODES), F32),
            jax.ShapeDtypeStruct((SPEC, CX, CY, CZ), F32),
        ),
        in_specs=[vmem, smem, vmem, vmem, smem, smem, smem, pl.BlockSpec(memory_space=pl.ANY)],
        out_specs=(vmem, vmem),
        scratch_shapes=[
            v((BASIS_ROWS, MODES), BF16),
            v((STEPS + 1, SPEC, CX, CY, CZ), F32),
            v((2, CX, CY, CZ), F32),
            v((2, 2, SPEC, 2, CY, CZ), F32),
            v((2, 2, SPEC, CX, 8, CZ), F32),
            v((2, 2, 8, CZ), F32),
            v((2, 6, 8, CZ), F32),
            v((2, 12, 8, CZ), F32),
            v((2, 2, 1, CY, CZ), F32),
            v((2, 2, CX, 8, CZ), F32),
            v((2, 2, CX, CY, CZ), F32),
            v((SPEC, 8, 24, 256), F32),
            v((SPEC, 6, 24, 256), F32),
            v((SPEC, 6, 24, 256), F32),
            v((6, 24, 256), F32),
            v((SPEC, 6, 24, 256), F32),
            v((SPEC, SPEC, 6, 24, 256), F32),
            v((MODES, MODES), F32),
            v((STEPS, 4, CX, CY, CZ), F32),
            v((2 * STEPS, MODES), F32),
            v((16, SNAPS, MODES), F32),
            v((8, SNAPS, MODES), F32),
            v((16, 16, MODES), F32),
            v((8, 16, MODES), F32),
            v((MODES, MODES), F32),
            dma((ROUNDS,)),
            dma((2, 18)),
            dma((2, 18)),
            dma((6,)),
            dma((6,)),
            dma((ROUNDS, 3)),
            dma((ROUNDS, 3)),
            dma((2, 16)),
            dma((2, 16)),
            dma((3, 16)),
            dma((3, 16)),
        ],
        compiler_params=pltpu.CompilerParams(
            collective_id=0, has_side_effects=True, vmem_limit_bytes=60 * 1024 * 1024
        ),
    )(
        terminal, diffusion, velocity, material, rates, stoich.T, plan,
        basis.reshape(BASIS_ROWS, MODES),
    )


def solution(mesh):
    return jax.shard_map(
        body,
        mesh=mesh,
        in_specs=(
            P(None, "gx", "gy", "grp"),
            P(),
            P("gx", "gy", "grp"),
            P("gx", "gy", "grp"),
            P(),
            P(),
            P(),
            P("grp", "gx", "gy", None, None),
        ),
        out_specs=(P(), P(None, "gx", "gy", "grp")),
        check_vma=False,
    )
```

```python
import jax
import jax.numpy as jnp
from jax import lax
from jax.experimental import pallas as pl
from jax.experimental.pallas import tpu as pltpu
from jax.sharding import PartitionSpec as P

SPEC = 4
MATS = 8
STEPS = 16
ROUNDS = STEPS // 2
SNAPS = 8
MODES = 256
CX, CY, CZ = 4, 16, 128
ROWS = CX * CY
BASIS_ROWS = ROWS * 512
PART = BASIS_ROWS // ROUNDS
MESH = pl.DeviceIdType.MESH
F32 = jnp.float32
BF16 = jnp.bfloat16

FACES = [(-1, 0, 0), (1, 0, 0), (0, -1, 0), (0, 1, 0), (0, 0, -1), (0, 0, 1)]
XZ = [(a, 0, b) for a in (-1, 1) for b in (-1, 1)]
XY = [(a, b, 0) for a in (-1, 1) for b in (-1, 1)]
YZ = [(0, a, b) for a in (-1, 1) for b in (-1, 1)]
DIRS = FACES + XZ + XY + YZ
ORDER = [6, 7, 8, 9, 10, 11, 12, 13, 0, 1, 14, 15, 16, 17, 4, 5, 2, 3]


def kernel(
    terminal_in, diffusion_in, velocity_in, material_in, rates_in, stoich_in, plan_in, basis,
    coeff_to, adj_to,
    diffusion, rates, stoich, plan, material, coeff_out, in_sem, out_sem, bv, st, fields, rx, ry, rz, pack, edge, cx, cy, cz, lam, mid,
    kc, vm, dm, rc, gram, got, proj, suma, sumb, gparts, gsums, gfull,
    basis_sem, hs, hr, cs, cr, as_, ar, ss, sr, gs, gr,
):
    g = lax.axis_index("grp")
    x = lax.axis_index("gx")
    y = lax.axis_index("gy")
    n_g, n_x, n_y = 4, 8, 4

    def has(d):
        cond = None
        for step, at, count in ((d[0], x, n_x), (d[1], y, n_y), (d[2], g, n_g)):
            if step == 0:
                continue
            term = at > 0 if step < 0 else at < count - 1
            cond = term if cond is None else jnp.logical_and(cond, term)
        return cond

    def minus(d):
        return tuple(-v for v in d)

    def dev(d):
        return (g + d[2], x + d[0], y + d[1])

    sub = lax.broadcasted_iota(jnp.int32, (8, CZ), 0)
    lane = lax.broadcasted_iota(jnp.int32, (8, CZ), 1)
    odd_lane = lax.rem(lane, 2) == 1
    odd_sub = lax.rem(sub, 2) == 1

    def low(cond, most):
        return jnp.where(cond, most, 0)

    def high(cond, least, size):
        return jnp.where(cond, least, size)

    def basis_copy(c):
        rows = pl.ds(c * PART, PART)
        return pltpu.make_async_copy(basis.at[rows, :], bv.at[rows, :], basis_sem.at[c])

    inputs = [
        pltpu.make_async_copy(src, dst, in_sem.at[i]) for i, (src, dst) in enumerate((
            (terminal_in, st.at[0]), (velocity_in, fields.at[0]), (material_in, material),
            (diffusion_in, diffusion), (rates_in, rates), (stoich_in, stoich),
            (plan_in, plan)))
    ]
    for copy in inputs:
        copy.start()
    for c in range(ROUNDS):
        basis_copy(c).start()


    barrier = pltpu.get_barrier_semaphore()
    ga = g * n_y + y

    def group_a(o):
        q = lax.rem(ga + o, n_g * n_y)
        return q, (q // n_y, x, lax.rem(q, n_y))

    def group_b(o):
        q = lax.rem(x + o, n_x)
        return q, (g, q, y)

    count = jnp.int32(n_g * n_y - 1 + n_x - 1)
    for o in range(1, n_g * n_y):
        pl.semaphore_signal(barrier, inc=1, device_id=group_a(o)[1], device_id_type=MESH)
    for o in range(1, n_x):
        pl.semaphore_signal(barrier, inc=1, device_id=group_b(o)[1], device_id_type=MESH)
    for d in XZ + XY:
        cond = has(d)
        count = count + cond.astype(jnp.int32)

        @pl.when(cond)
        def _(d=d):
            pl.semaphore_signal(barrier, inc=1, device_id=dev(d), device_id_type=MESH)

    lam[...] = jnp.zeros_like(lam)
    mid[...] = jnp.zeros_like(mid)
    gram[...] = jnp.zeros_like(gram)
    for copy in inputs:
        copy.wait()
    fields[1] = material[...].astype(F32)
    lam[:, 2:6, 0:16, 0:128] = st[0]
    pl.semaphore_wait(barrier, count)

    def halo_copy(i, k, par):
        d = DIRS[i]
        n = 2 * k
        if i < 2:
            src = st.at[n, :, pl.ds(0 if i == 0 else 2, 2)]
            dst = rx.at[par, i]
        elif i < 4:
            src = st.at[n, :, :, pl.ds(0 if i == 2 else 8, 8), :]
            dst = ry.at[par, i - 2]
        elif i < 6:
            src = pack.at[par, 5]
            dst = rz.at[par, i - 4]
        else:
            if i < 10:
                which = (i - 6) // 2
            elif i < 14:
                which = 2 + (i - 10) // 2
            else:
                which = 4
            src = pack.at[par, which]
            dst = edge.at[par, i - 6]
        return pltpu.make_async_remote_copy(
            src_ref=src, dst_ref=dst, send_sem=hs.at[par, i], recv_sem=hr.at[par, i],
            device_id=dev(d), device_id_type=MESH,
        )

    def pack_x_edges(k, par):
        n = 2 * k
        for side in (0, 1):
            plane = 0 if side == 0 else CX - 1
            acc = jnp.zeros((8, CZ), F32)
            rows = jnp.zeros((8, CZ), F32)
            for s in range(SPEC):
                t0 = st[n, s, plane, 0:8, :]
                t1 = st[n, s, plane, 8:16, :]
                for t, v in ((0, t0), (1, t1)):
                    i = 2 * (s * 2 + t)
                    hit = jnp.logical_or(lane == i, lane == (i - 1) % CZ)
                    acc = jnp.where(hit, pltpu.roll(v, i, 1) if i else v, acc)
                i = 2 * s
                both = jnp.where(sub < 4, t0, t1)
                hit = jnp.logical_or(sub == i, sub == (i - 1) % 8)
                rows = jnp.where(hit, pltpu.roll(both, i, 0) if i else both, rows)
            pack[par, side] = acc
            pack[par, 2 + side] = rows

    def pack_others(k, par):
        n = 2 * k
        acc = jnp.zeros((8, CZ), F32)
        face = jnp.zeros((8, CZ), F32)
        for s in range(SPEC):
            for p in range(CX):
                t0 = st[n, s, p, 0:8, :]
                t1 = st[n, s, p, 8:16, :]
                i = 2 * (s * CX + p)
                v = jnp.where(sub < 4, t0, t1)
                hit = jnp.logical_or(lane == i, lane == (i - 1) % CZ)
                acc = jnp.where(hit, pltpu.roll(v, i, 1) if i else v, acc)
                for t, v in ((0, t0), (1, t1)):
                    i = 4 * ((s * CX + p) * 2 + t)
                    place = lax.rem(lane + (CZ + 2 - i), CZ)
                    face = jnp.where(place < 4, pltpu.roll(v, i, 1) if i else v, face)
        pack[par, 4] = acc
        pack[par, 5] = face

    def send(i, k, par):
        @pl.when(has(DIRS[i]))
        def _():
            halo_copy(i, k, par).start()

    def start_halo(k, par):
        pack_x_edges(k, par)
        for i in ORDER[:10]:
            send(i, k, par)
        pack_others(k, par)
        for i in ORDER[10:]:
            send(i, k, par)

    def wait_halo(k, par):
        for i in ORDER:

            @pl.when(has(minus(DIRS[i])))
            def _(i=i):
                halo_copy(i, k, par).wait_recv()

    def wait_sent(k, par):
        for i in ORDER:

            @pl.when(has(DIRS[i]))
            def _(i=i):
                halo_copy(i, k, par).wait_send()

    xm, xp = has((-1, 0, 0)), has((1, 0, 0))
    ym, yp = has((0, -1, 0)), has((0, 1, 0))
    zm, zp = has((0, 0, -1)), has((0, 0, 1))
    y_from_p = sub < low(yp, 4)
    y_from_m = sub >= high(ym, 4, 8)
    lane_full = lax.broadcasted_iota(jnp.int32, (CY, CZ), 1)
    z_from_p = lane_full < low(zp, 64)
    z_from_m = lane_full >= high(zm, 64, CZ)

    def unpack(par):
        zero8 = jnp.zeros((8, CZ), F32)
        far = lax.rem(lane, 4) >= 2
        comb = jnp.where(
            jnp.logical_and(far, lane < low(zm, CZ)), rz[par, 1],
            jnp.where(
                jnp.logical_and(jnp.logical_not(far), lane < low(zp, CZ)), rz[par, 0], zero8))
        for s in range(SPEC):
            for p in range(CX):
                for t in range(2):
                    i = 4 * ((s * CX + p) * 2 + t)
                    tile = pltpu.roll(comb, (CZ - i) % CZ, 1) if i else comb
                    lam[s, 2 + p, t * 8:(t + 1) * 8, 128:256] = tile
        for s in range(SPEC):
            lam[s, 0:2, 0:16, 0:128] = jnp.where(xm, rx[par, 1, s], 0.0)
            lam[s, 6:8, 0:16, 0:128] = jnp.where(xp, rx[par, 0, s], 0.0)
            for p in range(CX):
                lam[s, 2 + p, 16:24, 0:128] = jnp.where(
                    y_from_p, ry[par, 0, s, p], jnp.where(y_from_m, ry[par, 1, s, p], zero8))

        def flag(a, b):
            return jnp.logical_and(a, b)

        for side, xh in ((1, xm), (0, xp)):
            base = side * 2
            m_m, m_p = edge[par, base + 1], edge[par, base]
            comb = jnp.where(
                jnp.logical_and(odd_lane, lane < low(flag(xh, zm), CZ)), m_m,
                jnp.where(
                    jnp.logical_and(jnp.logical_not(odd_lane), lane < low(flag(xh, zp), CZ)),
                    m_p, zero8))
            at = 1 if side == 1 else 6
            for s in range(SPEC):
                for t in range(2):
                    i = 2 * (s * 2 + t)
                    tile = pltpu.roll(comb, (CZ - i) % CZ, 1) if i else comb
                    lam[s, at, t * 8:(t + 1) * 8, 128:256] = tile
        for side, xh in ((1, xm), (0, xp)):
            base = 4 + side * 2
            m_m, m_p = edge[par, base + 1], edge[par, base]
            comb = jnp.where(
                jnp.logical_and(odd_sub, sub < low(flag(xh, ym), 8)), m_m,
                jnp.where(
                    jnp.logical_and(jnp.logical_not(odd_sub), sub < low(flag(xh, yp), 8)),
                    m_p, zero8))
            at = 1 if side == 1 else 6
            for s in range(SPEC):
                i = 2 * s
                tile = pltpu.roll(comb, (8 - i) % 8, 0) if i else comb
                lam[s, at, 16:24, 0:128] = tile
        even_lane = jnp.logical_not(odd_lane)
        hi_m = jnp.logical_and(odd_lane, sub >= high(flag(ym, zm), 4, 8))
        hi_p = jnp.logical_and(even_lane, sub >= high(flag(ym, zp), 4, 8))
        lo_m = jnp.logical_and(odd_lane, sub < low(flag(yp, zm), 4))
        lo_p = jnp.logical_and(even_lane, sub < low(flag(yp, zp), 4))
        comb = jnp.where(hi_m, edge[par, 11], zero8)
        comb = jnp.where(hi_p, edge[par, 10], comb)
        comb = jnp.where(lo_m, edge[par, 9], comb)
        comb = jnp.where(lo_p, edge[par, 8], comb)
        for s in range(SPEC):
            for p in range(CX):
                i = 2 * (s * CX + p)
                tile = pltpu.roll(comb, (CZ - i) % CZ, 1) if i else comb
                lam[s, 2 + p, 16:24, 128:256] = tile

    def coeff_copy(i):
        if i < 2:
            src = fields.at[:, pl.ds(0 if i == 0 else CX - 1, 1)]
            dst = cx.at[i]
        elif i < 4:
            src = fields.at[:, :, pl.ds(0 if i == 2 else 8, 8), :]
            dst = cy.at[i - 2]
        else:
            src = fields
            dst = cz.at[i - 4]
        return pltpu.make_async_remote_copy(
            src_ref=src, dst_ref=dst, send_sem=cs.at[i], recv_sem=cr.at[i],
            device_id=dev(DIRS[i]), device_id_type=MESH,
        )

    for i in range(6):

        @pl.when(has(DIRS[i]))
        def _(i=i):
            coeff_copy(i).start()

    def snap_copy(k, o):
        q = lax.rem(g + o, n_g)
        return pltpu.make_async_remote_copy(
            src_ref=st.at[pl.ds(2 * k + 1, 2), q],
            dst_ref=got.at[pl.ds(2 * k, 2), g],
            send_sem=as_.at[k, o - 1], recv_sem=ar.at[k, o - 1],
            device_id=(q, x, y), device_id_type=MESH,
        )


    def coefficients(outer):
        for p in range(6):
            own = 1 <= p <= CX
            for r0, r1, l0, l1 in ((0, 16, 0, 128), (16, 24, 0, 128), (0, 16, 128, 256)):
                if not own and (r0, l0) != (0, 0):
                    continue
                if outer == (own and (r0, l0) == (0, 0)):
                    continue
                vals = []
                for f in range(2):
                    if not own:
                        side, ok = (1, xm) if p == 0 else (0, xp)
                        v = jnp.where(ok, cx[side, f, 0], 0.0)
                    elif (r0, l0) == (0, 0):
                        v = fields[f, p - 1]
                    elif r0 == 16:
                        v = jnp.where(y_from_p, cy[0, f, p - 1],
                                      jnp.where(y_from_m, cy[1, f, p - 1], 0.0))
                    else:
                        v = jnp.where(z_from_p, cz[0, f, p - 1],
                                      jnp.where(z_from_m, cz[1, f, p - 1], 0.0))
                    vals.append(v)
                vel, mat = vals
                if not own:
                    ok = xm if p == 0 else xp
                    inside = jnp.where(ok, 1.0, 0.0) * jnp.ones((16, 128), F32)
                elif (r0, l0) == (0, 0):
                    inside = jnp.ones((16, 128), F32)
                elif r0 == 16:
                    inside = jnp.where(jnp.logical_or(y_from_p, y_from_m), 1.0, 0.0)
                else:
                    inside = jnp.where(jnp.logical_or(z_from_p, z_from_m), 1.0, 0.0)
                looked = []
                for r in range(8):
                    v = jnp.full(mat.shape, rates[0, r], F32)
                    for m in range(1, MATS):
                        v = jnp.where(mat == float(m), rates[m, r], v)
                    looked.append(v * inside)
                vel = vel * inside
                vm[p, r0:r1, l0:l1] = vel
                for a in range(SPEC):
                    dm[a, p, r0:r1, l0:l1] = inside * diffusion[a]
                    for b in range(SPEC):
                        v = (looked[a] * stoich[b, a].astype(F32)
                             + looked[a + 4] * stoich[b, a + 4].astype(F32))
                        if a == b:
                            kc[a, p, r0:r1, l0:l1] = (
                                inside * (1.0 - 6.0 * diffusion[a]) - vel + v)
                        else:
                            rc[a, b, p, r0:r1, l0:l1] = v

    def advance(cs_, s, p, tile, dn, up, ys, zs):
        r0, r1, l0, l1 = tile
        box = (p, slice(r0, r1), slice(l0, l1))
        total = dm[(s,) + box] * (((dn + up) + ys) + zs)
        total = total + kc[(s,) + box] * cs_[s]
        total = total + vm[box] * up
        for b in range(SPEC):
            if b != s:
                total = total + rc[(s, b) + box] * cs_[b]
        return total

    own_tile = (0, 16, 0, 128)

    def first_step():
        for p in range(6):
            full = [lam[s, p + 1] for s in range(SPEC)]
            for s in range(SPEC):
                c = full[s]
                ya = pltpu.roll(c, 1, 0) + pltpu.roll(c, 23, 0)
                za = pltpu.roll(c, 1, 1) + pltpu.roll(c, 255, 1)
                tiles = [own_tile]
                if 1 <= p <= CX:
                    tiles += [(16, 24, 0, 128), (0, 16, 128, 256)]
                for t in tiles:
                    r0, r1, l0, l1 = t
                    mid[s, p, r0:r1, l0:l1] = advance(
                        [v[r0:r1, l0:l1] for v in full], s, p, t,
                        lam[s, p, r0:r1, l0:l1], lam[s, p + 2, r0:r1, l0:l1],
                        ya[r0:r1, l0:l1], za[r0:r1, l0:l1])

    def second_step(n):
        for p in range(1, 1 + CX):
            own = [mid[s, p, 0:16, 0:128] for s in range(SPEC)]
            for s in range(SPEC):
                col = mid[s, p, :, 0:128]
                ya = (pltpu.roll(col, 1, 0) + pltpu.roll(col, 23, 0))[0:16]
                row = mid[s, p, 0:16, :]
                za = (pltpu.roll(row, 1, 1) + pltpu.roll(row, 255, 1))[:, 0:128]
                new = advance(own, s, p, own_tile, mid[s, p - 1, 0:16, 0:128],
                              mid[s, p + 1, 0:16, 0:128], ya, za)
                st[n + 1, s, p - 1] = own[s]
                st[n + 2, s, p - 1] = new
                lam[s, p + 1, 0:16, 0:128] = new

    def gram_part(k):
        rows = 512
        basis_copy(2 * k).wait()
        basis_copy(2 * k + 1).wait()

        def one(c, carry):
            at = pl.multiple_of(k * 2 * PART + c * rows, rows)
            block = bv[pl.ds(at, rows), :]
            gram[...] += lax.dot_general(
                block, block, (((0,), (0,)), ((), ())), preferred_element_type=F32)
            return carry

        lax.fori_loop(0, 2 * PART // rows, one, 0)

    slab = MODES // (n_g * n_y)

    def slab_of(q):
        return pl.ds(pl.multiple_of(q * slab, slab), slab)

    def gram_a(o):
        q, where = group_a(o)
        return pltpu.make_async_remote_copy(
            src_ref=gram.at[slab_of(q), :], dst_ref=gparts.at[ga],
            send_sem=gs.at[0, o], recv_sem=gr.at[0, o], device_id=where, device_id_type=MESH)

    def gram_b(o):
        q, where = group_b(o)
        return pltpu.make_async_remote_copy(
            src_ref=gsums.at[x], dst_ref=gsums.at[x],
            send_sem=gs.at[1, o], recv_sem=gr.at[1, o], device_id=where, device_id_type=MESH)

    def gram_c(o):
        q, where = group_a(o)
        return pltpu.make_async_remote_copy(
            src_ref=gfull.at[slab_of(ga), :], dst_ref=gfull.at[slab_of(ga), :],
            send_sem=gs.at[2, o], recv_sem=gr.at[2, o], device_id=where, device_id_type=MESH)

    def gram_start():
        gparts[ga] = gram[slab_of(ga), :]
        for o in range(1, n_g * n_y):
            gram_a(o).start()

    def gram_middle():
        for o in range(1, n_g * n_y):
            gram_a(o).wait_recv()
        total = gparts[0]
        for q in range(1, n_g * n_y):
            total = total + gparts[q]
        gsums[x] = total
        for o in range(1, n_x):
            gram_b(o).start()

    def gram_last():
        for o in range(1, n_x):
            gram_b(o).wait_recv()
        total = gsums[0]
        for q in range(1, n_x):
            total = total + gsums[q]
        gfull[slab_of(ga), :] = total
        for o in range(1, n_g * n_y):
            gram_c(o).start()

    start_halo(0, 0)
    coefficients(False)
    gram_part(0)
    for i in range(6):

        @pl.when(has(minus(DIRS[i])))
        def _(i=i):
            coeff_copy(i).wait_recv()

    coefficients(True)

    def round_(k, carry):
        par = lax.rem(k, 2)

        @pl.when(k > 0)
        def _():
            start_halo(k, par)
            for o in range(1, n_g):
                snap_copy(k - 1, o).start()

        @pl.when(jnp.logical_and(k > 0, k < ROUNDS // 2))
        def _():
            gram_part(k)

        @pl.when(k == ROUNDS // 2)
        def _():
            gram_start()

        @pl.when(k == ROUNDS // 2 + 1)
        def _():
            gram_middle()

        @pl.when(k == ROUNDS // 2 + 2)
        def _():
            gram_last()

        wait_halo(k, par)
        unpack(par)
        first_step()
        second_step(2 * k)
        wait_sent(k, par)
        got[pl.ds(2 * k, 2), g] = st[pl.ds(2 * k + 1, 2), g]
        return carry

    lax.fori_loop(0, ROUNDS, round_, 0)
    for o in range(1, n_g):
        snap_copy(ROUNDS - 1, o).start()
    adj_copy = pltpu.make_async_copy(st.at[STEPS], adj_to, out_sem.at[0])
    adj_copy.start()
    for i in range(6):

        @pl.when(has(DIRS[i]))
        def _(i=i):
            coeff_copy(i).wait_send()

    flat = got.reshape(STEPS * 4 * ROWS, CZ)
    proj[...] = jnp.zeros_like(proj)
    unroll = 8

    def project(zq):
        def one(c, carry):
            vals, blocks = [], []
            for u in range(unroll):
                at = c * unroll + u
                vals.append(flat[pl.ds(zq * ROWS + at, STEPS, stride=4 * ROWS), :])
                blocks.append(
                    bv[pl.ds(pl.multiple_of(at * 512 + zq * CZ, CZ), CZ), :])
            a = jnp.concatenate(vals, axis=1)
            hi = a.astype(BF16)
            lo = (a - hi.astype(F32)).astype(BF16)
            both = jnp.concatenate([hi, lo], axis=0)
            proj[...] += jnp.dot(
                both, jnp.concatenate(blocks, axis=0), preferred_element_type=F32)
            return carry

        lax.fori_loop(0, ROWS // unroll, one, 0)

    project(g)
    for o in (1, 3, 2):
        def snap_wait(k, carry, o=o):
            snap_copy(k, o).wait_recv()
            return carry

        lax.fori_loop(0, ROUNDS, snap_wait, 0)
        project(lax.rem(g + n_g - o, n_g))

    slot = lax.broadcasted_iota(jnp.int32, (SNAPS, MODES), 0)
    step_of = jnp.zeros((SNAPS, MODES), jnp.int32)
    for j in range(SNAPS):
        step_of = jnp.where(slot == j, plan[j], step_of)
    first = jnp.zeros((SNAPS, MODES), F32)
    for n in range(STEPS):
        row = proj[n:n + 1, :] + proj[STEPS + n:STEPS + n + 1, :]
        first = jnp.where(step_of == n, jnp.broadcast_to(row, first.shape), first)

    def all_sum(value):
        suma[ga] = value

        def a_copy(o):
            q, where = group_a(o)
            return pltpu.make_async_remote_copy(
                src_ref=suma.at[ga], dst_ref=suma.at[ga],
                send_sem=ss.at[0, o], recv_sem=sr.at[0, o],
                device_id=where, device_id_type=MESH)

        def b_copy(o):
            q, where = group_b(o)
            return pltpu.make_async_remote_copy(
                src_ref=sumb.at[x], dst_ref=sumb.at[x],
                send_sem=ss.at[1, o], recv_sem=sr.at[1, o],
                device_id=where, device_id_type=MESH)

        for o in range(1, n_g * n_y):
            a_copy(o).start()
        for o in range(1, n_g * n_y):
            a_copy(o).wait_recv()
        total = suma[0]
        for q in range(1, n_g * n_y):
            total = total + suma[q]
        sumb[x] = total
        for o in range(1, n_x):
            b_copy(o).start()
        for o in range(1, n_x):
            b_copy(o).wait_recv()
        total = sumb[0]
        for q in range(1, n_x):
            total = total + sumb[q]

        def finish():
            for o in range(1, n_g * n_y):
                a_copy(o).wait_send()
            for o in range(1, n_x):
                b_copy(o).wait_send()

        return total, finish

    total, finish = all_sum(first)
    low_first = total.astype(BF16)
    for o in range(1, n_g * n_y):
        gram_c(o).wait_recv()
    gm = gfull[...]
    g1 = gm.astype(BF16)
    left = gm - g1.astype(F32)
    g2 = left.astype(BF16)
    g3 = (left - g2.astype(F32)).astype(BF16)
    back = jnp.dot(low_first, g1, preferred_element_type=F32)
    back += jnp.dot(low_first, g2, preferred_element_type=F32)
    back += jnp.dot(low_first, g3, preferred_element_type=F32)
    coeff_out[...] = total + (total - back)
    coeff_copy_out = pltpu.make_async_copy(coeff_out, coeff_to, out_sem.at[1])
    coeff_copy_out.start()
    finish()
    for o in range(1, n_g * n_y):
        gram_a(o).wait_send()
        gram_c(o).wait_send()
    for o in range(1, n_x):
        gram_b(o).wait_send()

    def snap_sent(k, carry):
        for o in range(1, n_g):
            snap_copy(k, o).wait_send()
        return carry

    lax.fori_loop(0, ROUNDS, snap_sent, 0)
    adj_copy.wait()
    coeff_copy_out.wait()


def body(terminal, diffusion, velocity, material, rates, stoich, plan, basis):
    sm = pltpu.SMEM
    dma = pltpu.SemaphoreType.DMA
    v = pltpu.VMEM
    return pl.pallas_call(
        kernel,
        out_shape=(
            jax.ShapeDtypeStruct((SNAPS, MODES), F32),
            jax.ShapeDtypeStruct((SPEC, CX, CY, CZ), F32),
        ),
        in_specs=[pl.BlockSpec(memory_space=pl.ANY)] * 8,
        out_specs=(pl.BlockSpec(memory_space=pl.ANY),) * 2,
        scratch_shapes=[
            sm((SPEC,), F32),
            sm((MATS, 8), F32),
            sm((SPEC, 8), jnp.int32),
            sm((SNAPS,), jnp.int32),
            v((CX, CY, CZ), jnp.int32),
            v((SNAPS, MODES), F32),
            dma((7,)),
            dma((2,)),
            v((BASIS_ROWS, MODES), BF16),
            v((STEPS + 1, SPEC, CX, CY, CZ), F32),
            v((2, CX, CY, CZ), F32),
            v((2, 2, SPEC, 2, CY, CZ), F32),
            v((2, 2, SPEC, CX, 8, CZ), F32),
            v((2, 2, 8, CZ), F32),
            v((2, 6, 8, CZ), F32),
            v((2, 12, 8, CZ), F32),
            v((2, 2, 1, CY, CZ), F32),
            v((2, 2, CX, 8, CZ), F32),
            v((2, 2, CX, CY, CZ), F32),
            v((SPEC, 8, 24, 256), F32),
            v((SPEC, 6, 24, 256), F32),
            v((SPEC, 6, 24, 256), F32),
            v((6, 24, 256), F32),
            v((SPEC, 6, 24, 256), F32),
            v((SPEC, SPEC, 6, 24, 256), F32),
            v((MODES, MODES), F32),
            v((STEPS, 4, CX, CY, CZ), F32),
            v((2 * STEPS, MODES), F32),
            v((16, SNAPS, MODES), F32),
            v((8, SNAPS, MODES), F32),
            v((16, 16, MODES), F32),
            v((8, 16, MODES), F32),
            v((MODES, MODES), F32),
            dma((ROUNDS,)),
            dma((2, 18)),
            dma((2, 18)),
            dma((6,)),
            dma((6,)),
            dma((ROUNDS, 3)),
            dma((ROUNDS, 3)),
            dma((2, 16)),
            dma((2, 16)),
            dma((3, 16)),
            dma((3, 16)),
        ],
        compiler_params=pltpu.CompilerParams(
            collective_id=0, has_side_effects=True, vmem_limit_bytes=60 * 1024 * 1024
        ),
    )(
        terminal, diffusion, velocity, material, rates, stoich.T, plan,
        basis.reshape(BASIS_ROWS, MODES),
    )


def solution(mesh):
    return jax.shard_map(
        body,
        mesh=mesh,
        in_specs=(
            P(None, "gx", "gy", "grp"),
            P(),
            P("gx", "gy", "grp"),
            P("gx", "gy", "grp"),
            P(),
            P(),
            P(),
            P("grp", "gx", "gy", None, None),
        ),
        out_specs=(P(), P(None, "gx", "gy", "grp")),
        check_vma=False,
    )
```

```python
import jax
import jax.numpy as jnp
from jax import lax
from jax.experimental import pallas as pl
from jax.experimental.pallas import tpu as pltpu
from jax.sharding import PartitionSpec as P

SPEC = 4
MATS = 8
STEPS = 16
ROUNDS = STEPS // 2
SNAPS = 8
MODES = 256
CX, CY, CZ = 4, 16, 128
ROWS = CX * CY
BASIS_ROWS = ROWS * 512
PART = BASIS_ROWS // ROUNDS
MESH = pl.DeviceIdType.MESH
F32 = jnp.float32
BF16 = jnp.bfloat16

FACES = [(-1, 0, 0), (1, 0, 0), (0, -1, 0), (0, 1, 0), (0, 0, -1), (0, 0, 1)]
XZ = [(a, 0, b) for a in (-1, 1) for b in (-1, 1)]
XY = [(a, b, 0) for a in (-1, 1) for b in (-1, 1)]
YZ = [(0, a, b) for a in (-1, 1) for b in (-1, 1)]
DIRS = FACES + XZ + XY + YZ
ORDER = [6, 7, 8, 9, 10, 11, 12, 13, 0, 1, 14, 15, 16, 17, 4, 5, 2, 3]


def kernel(
    terminal_in, diffusion_in, velocity_in, material_in, rates_in, stoich_in, plan_in, basis,
    coeff_to, adj_to,
    diffusion, rates, stoich, plan, material, coeff_out, in_sem, out_sem, bv, st, fields, rx, ry, rz, pack, edge, cx, cy, cz, lam, mid,
    kc, vm, dm, rc, gram, got, proj, suma, sumb, gparts, gsums, gfull,
    basis_sem, hs, hr, cs, cr, as_, ar, ss, sr, gs, gr,
):
    g = lax.axis_index("grp")
    x = lax.axis_index("gx")
    y = lax.axis_index("gy")
    n_g, n_x, n_y = 4, 8, 4

    def has(d):
        cond = None
        for step, at, count in ((d[0], x, n_x), (d[1], y, n_y), (d[2], g, n_g)):
            if step == 0:
                continue
            term = at > 0 if step < 0 else at < count - 1
            cond = term if cond is None else jnp.logical_and(cond, term)
        return cond

    def minus(d):
        return tuple(-v for v in d)

    def dev(d):
        return (g + d[2], x + d[0], y + d[1])

    sub = lax.broadcasted_iota(jnp.int32, (8, CZ), 0)
    lane = lax.broadcasted_iota(jnp.int32, (8, CZ), 1)
    odd_lane = lax.rem(lane, 2) == 1
    odd_sub = lax.rem(sub, 2) == 1

    def low(cond, most):
        return jnp.where(cond, most, 0)

    def high(cond, least, size):
        return jnp.where(cond, least, size)

    def basis_copy(c):
        rows = pl.ds(c * PART, PART)
        return pltpu.make_async_copy(basis.at[rows, :], bv.at[rows, :], basis_sem.at[c])

    inputs = [
        pltpu.make_async_copy(src, dst, in_sem.at[i]) for i, (src, dst) in enumerate((
            (terminal_in, st.at[0]), (velocity_in, fields.at[0]), (material_in, material),
            (diffusion_in, diffusion), (rates_in, rates), (stoich_in, stoich),
            (plan_in, plan)))
    ]
    for copy in inputs:
        copy.start()
    for c in range(ROUNDS):
        basis_copy(c).start()


    barrier = pltpu.get_barrier_semaphore()
    ga = g * n_y + y

    def group_a(o):
        q = lax.rem(ga + o, n_g * n_y)
        return q, (q // n_y, x, lax.rem(q, n_y))

    def group_b(o):
        q = lax.rem(x + o, n_x)
        return q, (g, q, y)

    count = jnp.int32(n_g * n_y - 1 + n_x - 1)
    for d in XZ + XY:
        cond = has(d)
        count = count + cond.astype(jnp.int32)

        @pl.when(cond)
        def _(d=d):
            pl.semaphore_signal(barrier, inc=1, device_id=dev(d), device_id_type=MESH)

    for o in (4, 3, 5, 2, 6, 1, 7):
        pl.semaphore_signal(barrier, inc=1, device_id=group_b(o)[1], device_id_type=MESH)
    for o in range(1, n_g * n_y):
        pl.semaphore_signal(barrier, inc=1, device_id=group_a(o)[1], device_id_type=MESH)

    lam[...] = jnp.zeros_like(lam)
    mid[...] = jnp.zeros_like(mid)
    gram[...] = jnp.zeros_like(gram)
    for copy in inputs:
        copy.wait()
    fields[1] = material[...].astype(F32)
    lam[:, 2:6, 0:16, 0:128] = st[0]
    pl.semaphore_wait(barrier, count)

    def halo_copy(i, k, par):
        d = DIRS[i]
        n = 2 * k
        if i < 2:
            src = st.at[n, :, pl.ds(0 if i == 0 else 2, 2)]
            dst = rx.at[par, i]
        elif i < 4:
            src = st.at[n, :, :, pl.ds(0 if i == 2 else 8, 8), :]
            dst = ry.at[par, i - 2]
        elif i < 6:
            src = pack.at[par, 5]
            dst = rz.at[par, i - 4]
        else:
            if i < 10:
                which = (i - 6) // 2
            elif i < 14:
                which = 2 + (i - 10) // 2
            else:
                which = 4
            src = pack.at[par, which]
            dst = edge.at[par, i - 6]
        return pltpu.make_async_remote_copy(
            src_ref=src, dst_ref=dst, send_sem=hs.at[par, i], recv_sem=hr.at[par, i],
            device_id=dev(d), device_id_type=MESH,
        )

    def pack_x_edges(k, par):
        n = 2 * k
        for side in (0, 1):
            plane = 0 if side == 0 else CX - 1
            acc = jnp.zeros((8, CZ), F32)
            rows = jnp.zeros((8, CZ), F32)
            for s in range(SPEC):
                t0 = st[n, s, plane, 0:8, :]
                t1 = st[n, s, plane, 8:16, :]
                for t, v in ((0, t0), (1, t1)):
                    i = 2 * (s * 2 + t)
                    hit = jnp.logical_or(lane == i, lane == (i - 1) % CZ)
                    acc = jnp.where(hit, pltpu.roll(v, i, 1) if i else v, acc)
                i = 2 * s
                both = jnp.where(sub < 4, t0, t1)
                hit = jnp.logical_or(sub == i, sub == (i - 1) % 8)
                rows = jnp.where(hit, pltpu.roll(both, i, 0) if i else both, rows)
            pack[par, side] = acc
            pack[par, 2 + side] = rows

    def pack_others(k, par):
        n = 2 * k
        acc = jnp.zeros((8, CZ), F32)
        face = jnp.zeros((8, CZ), F32)
        for s in range(SPEC):
            for p in range(CX):
                t0 = st[n, s, p, 0:8, :]
                t1 = st[n, s, p, 8:16, :]
                i = 2 * (s * CX + p)
                v = jnp.where(sub < 4, t0, t1)
                hit = jnp.logical_or(lane == i, lane == (i - 1) % CZ)
                acc = jnp.where(hit, pltpu.roll(v, i, 1) if i else v, acc)
                for t, v in ((0, t0), (1, t1)):
                    i = 4 * ((s * CX + p) * 2 + t)
                    place = lax.rem(lane + (CZ + 2 - i), CZ)
                    face = jnp.where(place < 4, pltpu.roll(v, i, 1) if i else v, face)
        pack[par, 4] = acc
        pack[par, 5] = face

    def send(i, k, par):
        @pl.when(has(DIRS[i]))
        def _():
            halo_copy(i, k, par).start()

    def start_halo(k, par):
        pack_x_edges(k, par)
        for i in ORDER[:10]:
            send(i, k, par)
        pack_others(k, par)
        for i in ORDER[10:]:
            send(i, k, par)

    def wait_halo(k, par, which):
        for i in which:

            @pl.when(has(minus(DIRS[i])))
            def _(i=i):
                halo_copy(i, k, par).wait_recv()

    def wait_sent(k, par):
        for i in ORDER:

            @pl.when(has(DIRS[i]))
            def _(i=i):
                halo_copy(i, k, par).wait_send()

    xm, xp = has((-1, 0, 0)), has((1, 0, 0))
    ym, yp = has((0, -1, 0)), has((0, 1, 0))
    zm, zp = has((0, 0, -1)), has((0, 0, 1))
    y_from_p = sub < low(yp, 4)
    y_from_m = sub >= high(ym, 4, 8)
    lane_full = lax.broadcasted_iota(jnp.int32, (CY, CZ), 1)
    z_from_p = lane_full < low(zp, 64)
    z_from_m = lane_full >= high(zm, 64, CZ)

    def flag(a, b):
        return jnp.logical_and(a, b)

    even_lane = jnp.logical_not(odd_lane)
    zero8 = jnp.zeros((8, CZ), F32)

    def unpack_yz(par):
        far = lax.rem(lane, 4) >= 2
        comb = jnp.where(
            flag(far, lane < low(zm, CZ)), rz[par, 1],
            jnp.where(flag(jnp.logical_not(far), lane < low(zp, CZ)), rz[par, 0], zero8))
        hi_m = flag(odd_lane, sub >= high(flag(ym, zm), 4, 8))
        hi_p = flag(even_lane, sub >= high(flag(ym, zp), 4, 8))
        lo_m = flag(odd_lane, sub < low(flag(yp, zm), 4))
        lo_p = flag(even_lane, sub < low(flag(yp, zp), 4))
        corner = jnp.where(hi_m, edge[par, 11], zero8)
        corner = jnp.where(hi_p, edge[par, 10], corner)
        corner = jnp.where(lo_m, edge[par, 9], corner)
        corner = jnp.where(lo_p, edge[par, 8], corner)
        for s in range(SPEC):
            for p in range(CX):
                lam[s, 2 + p, 16:24, 0:128] = jnp.where(
                    y_from_p, ry[par, 0, s, p], jnp.where(y_from_m, ry[par, 1, s, p], zero8))
                for t in range(2):
                    i = 4 * ((s * CX + p) * 2 + t)
                    tile = pltpu.roll(comb, (CZ - i) % CZ, 1) if i else comb
                    lam[s, 2 + p, t * 8:(t + 1) * 8, 128:256] = tile
                i = 2 * (s * CX + p)
                tile = pltpu.roll(corner, (CZ - i) % CZ, 1) if i else corner
                lam[s, 2 + p, 16:24, 128:256] = tile

    def unpack_x(par):
        for s in range(SPEC):
            lam[s, 0:2, 0:16, 0:128] = jnp.where(xm, rx[par, 1, s], 0.0)
            lam[s, 6:8, 0:16, 0:128] = jnp.where(xp, rx[par, 0, s], 0.0)
        for side, xh in ((1, xm), (0, xp)):
            at = 1 if side == 1 else 6
            base = side * 2
            comb = jnp.where(
                flag(odd_lane, lane < low(flag(xh, zm), CZ)), edge[par, base + 1],
                jnp.where(
                    flag(even_lane, lane < low(flag(xh, zp), CZ)), edge[par, base], zero8))
            base = 4 + side * 2
            rows = jnp.where(
                flag(odd_sub, sub < low(flag(xh, ym), 8)), edge[par, base + 1],
                jnp.where(
                    flag(jnp.logical_not(odd_sub), sub < low(flag(xh, yp), 8)),
                    edge[par, base], zero8))
            for s in range(SPEC):
                for t in range(2):
                    i = 2 * (s * 2 + t)
                    tile = pltpu.roll(comb, (CZ - i) % CZ, 1) if i else comb
                    lam[s, at, t * 8:(t + 1) * 8, 128:256] = tile
                i = 2 * s
                tile = pltpu.roll(rows, (8 - i) % 8, 0) if i else rows
                lam[s, at, 16:24, 0:128] = tile

    def coeff_copy(i):
        if i < 2:
            src = fields.at[:, pl.ds(0 if i == 0 else CX - 1, 1)]
            dst = cx.at[i]
        elif i < 4:
            src = fields.at[:, :, pl.ds(0 if i == 2 else 8, 8), :]
            dst = cy.at[i - 2]
        else:
            src = fields
            dst = cz.at[i - 4]
        return pltpu.make_async_remote_copy(
            src_ref=src, dst_ref=dst, send_sem=cs.at[i], recv_sem=cr.at[i],
            device_id=dev(DIRS[i]), device_id_type=MESH,
        )

    def snap_copy(k, o):
        q = lax.rem(g + o, n_g)
        return pltpu.make_async_remote_copy(
            src_ref=st.at[pl.ds(2 * k + 1, 2), q],
            dst_ref=got.at[pl.ds(2 * k, 2), g],
            send_sem=as_.at[k, o - 1], recv_sem=ar.at[k, o - 1],
            device_id=(q, x, y), device_id_type=MESH,
        )


    def coefficients(outer):
        for p in range(6):
            own = 1 <= p <= CX
            for r0, r1, l0, l1 in ((0, 16, 0, 128), (16, 24, 0, 128), (0, 16, 128, 256)):
                if not own and (r0, l0) != (0, 0):
                    continue
                if outer == (own and (r0, l0) == (0, 0)):
                    continue
                vals = []
                for f in range(2):
                    if not own:
                        side, ok = (1, xm) if p == 0 else (0, xp)
                        v = jnp.where(ok, cx[side, f, 0], 0.0)
                    elif (r0, l0) == (0, 0):
                        v = fields[f, p - 1]
                    elif r0 == 16:
                        v = jnp.where(y_from_p, cy[0, f, p - 1],
                                      jnp.where(y_from_m, cy[1, f, p - 1], 0.0))
                    else:
                        v = jnp.where(z_from_p, cz[0, f, p - 1],
                                      jnp.where(z_from_m, cz[1, f, p - 1], 0.0))
                    vals.append(v)
                vel, mat = vals
                if not own:
                    ok = xm if p == 0 else xp
                    inside = jnp.where(ok, 1.0, 0.0) * jnp.ones((16, 128), F32)
                elif (r0, l0) == (0, 0):
                    inside = jnp.ones((16, 128), F32)
                elif r0 == 16:
                    inside = jnp.where(jnp.logical_or(y_from_p, y_from_m), 1.0, 0.0)
                else:
                    inside = jnp.where(jnp.logical_or(z_from_p, z_from_m), 1.0, 0.0)
                looked = []
                for r in range(8):
                    v = jnp.full(mat.shape, rates[0, r], F32)
                    for m in range(1, MATS):
                        v = jnp.where(mat == float(m), rates[m, r], v)
                    looked.append(v * inside)
                vel = vel * inside
                vm[p, r0:r1, l0:l1] = vel
                for a in range(SPEC):
                    dm[a, p, r0:r1, l0:l1] = inside * diffusion[a]
                    for b in range(SPEC):
                        v = (looked[a] * stoich[b, a].astype(F32)
                             + looked[a + 4] * stoich[b, a + 4].astype(F32))
                        if a == b:
                            kc[a, p, r0:r1, l0:l1] = (
                                inside * (1.0 - 6.0 * diffusion[a]) - vel + v)
                        else:
                            rc[a, b, p, r0:r1, l0:l1] = v

    def advance(cs_, s, p, tile, dn, up, ys, zs):
        r0, r1, l0, l1 = tile
        box = (p, slice(r0, r1), slice(l0, l1))
        total = dm[(s,) + box] * (((dn + up) + ys) + zs)
        total = total + kc[(s,) + box] * cs_[s]
        total = total + vm[box] * up
        for b in range(SPEC):
            if b != s:
                total = total + rc[(s, b) + box] * cs_[b]
        return total

    own_tile = (0, 16, 0, 128)

    def first_step(planes):
        for p in planes:
            full = [lam[s, p + 1] for s in range(SPEC)]
            for s in range(SPEC):
                c = full[s]
                ya = pltpu.roll(c, 1, 0) + pltpu.roll(c, 23, 0)
                za = pltpu.roll(c, 1, 1) + pltpu.roll(c, 255, 1)
                tiles = [own_tile]
                if 1 <= p <= CX:
                    tiles += [(16, 24, 0, 128), (0, 16, 128, 256)]
                for t in tiles:
                    r0, r1, l0, l1 = t
                    mid[s, p, r0:r1, l0:l1] = advance(
                        [v[r0:r1, l0:l1] for v in full], s, p, t,
                        lam[s, p, r0:r1, l0:l1], lam[s, p + 2, r0:r1, l0:l1],
                        ya[r0:r1, l0:l1], za[r0:r1, l0:l1])

    def second_step(n):
        for p in range(1, 1 + CX):
            own = [mid[s, p, 0:16, 0:128] for s in range(SPEC)]
            for s in range(SPEC):
                col = mid[s, p, :, 0:128]
                ya = (pltpu.roll(col, 1, 0) + pltpu.roll(col, 23, 0))[0:16]
                row = mid[s, p, 0:16, :]
                za = (pltpu.roll(row, 1, 1) + pltpu.roll(row, 255, 1))[:, 0:128]
                new = advance(own, s, p, own_tile, mid[s, p - 1, 0:16, 0:128],
                              mid[s, p + 1, 0:16, 0:128], ya, za)
                st[n + 1, s, p - 1] = own[s]
                st[n + 2, s, p - 1] = new
                lam[s, p + 1, 0:16, 0:128] = new

    block_rows = 1024

    def gram_blocks(start, count):
        def one(c, carry):
            at = pl.multiple_of((start + c) * block_rows, block_rows)
            block = bv[pl.ds(at, block_rows), :]
            gram[...] += lax.dot_general(
                block, block, (((0,), (0,)), ((), ())), preferred_element_type=F32)
            return carry

        lax.fori_loop(0, count, one, 0)

    slab = MODES // (n_g * n_y)

    def slab_of(q):
        return pl.ds(pl.multiple_of(q * slab, slab), slab)

    def gram_a(o):
        q, where = group_a(o)
        return pltpu.make_async_remote_copy(
            src_ref=gram.at[slab_of(q), :], dst_ref=gparts.at[ga],
            send_sem=gs.at[0, o], recv_sem=gr.at[0, o], device_id=where, device_id_type=MESH)

    def gram_b(o):
        q, where = group_b(o)
        return pltpu.make_async_remote_copy(
            src_ref=gsums.at[x], dst_ref=gsums.at[x],
            send_sem=gs.at[1, o], recv_sem=gr.at[1, o], device_id=where, device_id_type=MESH)

    def gram_c(o):
        q, where = group_a(o)
        return pltpu.make_async_remote_copy(
            src_ref=gfull.at[slab_of(ga), :], dst_ref=gfull.at[slab_of(ga), :],
            send_sem=gs.at[2, o], recv_sem=gr.at[2, o], device_id=where, device_id_type=MESH)

    def gram_start():
        gparts[ga] = gram[slab_of(ga), :]
        for o in range(1, n_g * n_y):
            gram_a(o).start()

    def gram_middle():
        for o in range(1, n_g * n_y):
            gram_a(o).wait_recv()
        total = gparts[0]
        for q in range(1, n_g * n_y):
            total = total + gparts[q]
        gsums[x] = total
        for o in range(1, n_x):
            gram_b(o).start()

    def gram_last():
        for o in range(1, n_x):
            gram_b(o).wait_recv()
        total = gsums[0]
        for q in range(1, n_x):
            total = total + gsums[q]
        gfull[slab_of(ga), :] = total
        for o in range(1, n_g * n_y):
            gram_c(o).start()

    start_halo(0, 0)
    for i in range(6):

        @pl.when(has(DIRS[i]))
        def _(i=i):
            coeff_copy(i).start()

    coefficients(False)
    for c in range(2):
        basis_copy(c).wait()
    gram_blocks(0, 8)
    for i in range(6):

        @pl.when(has(minus(DIRS[i])))
        def _(i=i):
            coeff_copy(i).wait_recv()

    coefficients(True)

    def round_(k, carry):
        par = lax.rem(k, 2)

        @pl.when(k > 0)
        def _():
            start_halo(k, par)
            for o in range(1, n_g):
                snap_copy(k - 1, o).start()

        @pl.when(k == 1)
        def _():
            for c in range(2, ROUNDS):
                basis_copy(c).wait()

        @pl.when(jnp.logical_and(k > 0, k < 5))
        def _():
            gram_blocks(2 + 6 * k, 6)

        @pl.when(k == 5)
        def _():
            gram_start()

        @pl.when(k == 6)
        def _():
            gram_middle()

        @pl.when(k == 7)
        def _():
            gram_last()

        wait_halo(k, par, ORDER[10:])
        unpack_yz(par)
        first_step((2, 3))
        wait_halo(k, par, ORDER[:10])
        unpack_x(par)
        first_step((0, 1, 4, 5))
        second_step(2 * k)
        wait_sent(k, par)
        got[pl.ds(2 * k, 2), g] = st[pl.ds(2 * k + 1, 2), g]
        return carry

    lax.fori_loop(0, ROUNDS, round_, 0)
    for o in (2, 1, 3):
        snap_copy(ROUNDS - 1, o).start()
    adj_copy = pltpu.make_async_copy(st.at[STEPS], adj_to, out_sem.at[0])
    adj_copy.start()
    for i in range(6):

        @pl.when(has(DIRS[i]))
        def _(i=i):
            coeff_copy(i).wait_send()

    flat = got.reshape(STEPS * 4 * ROWS, CZ)
    proj[...] = jnp.zeros_like(proj)
    unroll = 16

    def project(zq):
        def one(c, total):
            vals, blocks = [], []
            for u in range(unroll):
                at = c * unroll + u
                vals.append(flat[pl.ds(zq * ROWS + at, STEPS, stride=4 * ROWS), :])
                blocks.append(
                    bv[pl.ds(pl.multiple_of(at * 512 + zq * CZ, CZ), CZ), :])
            a = jnp.concatenate(vals, axis=1)
            hi = a.astype(BF16)
            lo = (a - hi.astype(F32)).astype(BF16)
            both = jnp.concatenate([hi, lo], axis=0)
            return total + jnp.dot(
                both, jnp.concatenate(blocks, axis=0), preferred_element_type=F32)

        proj[...] = lax.fori_loop(0, ROWS // unroll, one, proj[...])

    project(g)
    for o in (1, 3, 2):
        def snap_wait(k, carry, o=o):
            snap_copy(k, o).wait_recv()
            return carry

        lax.fori_loop(0, ROUNDS, snap_wait, 0)
        project(lax.rem(g + n_g - o, n_g))

    slot = lax.broadcasted_iota(jnp.int32, (SNAPS, MODES), 0)
    step_of = jnp.zeros((SNAPS, MODES), jnp.int32)
    for j in range(SNAPS):
        step_of = jnp.where(slot == j, plan[j], step_of)
    first = jnp.zeros((SNAPS, MODES), F32)
    for n in range(STEPS):
        row = proj[n:n + 1, :] + proj[STEPS + n:STEPS + n + 1, :]
        first = jnp.where(step_of == n, jnp.broadcast_to(row, first.shape), first)

    def all_sum(value):
        suma[ga] = value

        def a_copy(o):
            q, where = group_a(o)
            return pltpu.make_async_remote_copy(
                src_ref=suma.at[ga], dst_ref=suma.at[ga],
                send_sem=ss.at[0, o], recv_sem=sr.at[0, o],
                device_id=where, device_id_type=MESH)

        def b_copy(o):
            q, where = group_b(o)
            return pltpu.make_async_remote_copy(
                src_ref=sumb.at[x], dst_ref=sumb.at[x],
                send_sem=ss.at[1, o], recv_sem=sr.at[1, o],
                device_id=where, device_id_type=MESH)

        for o in range(1, n_g * n_y):
            a_copy(o).start()
        for o in range(1, n_g * n_y):
            a_copy(o).wait_recv()
        total = suma[0]
        for q in range(1, n_g * n_y):
            total = total + suma[q]
        sumb[x] = total
        for o in range(1, n_x):
            b_copy(o).start()
        for o in range(1, n_x):
            b_copy(o).wait_recv()
        total = sumb[0]
        for q in range(1, n_x):
            total = total + sumb[q]

        def finish():
            for o in range(1, n_g * n_y):
                a_copy(o).wait_send()
            for o in range(1, n_x):
                b_copy(o).wait_send()

        return total, finish

    total, finish = all_sum(first)
    low_first = total.astype(BF16)
    for o in range(1, n_g * n_y):
        gram_c(o).wait_recv()
    gm = gfull[...]
    g1 = gm.astype(BF16)
    left = gm - g1.astype(F32)
    g2 = left.astype(BF16)
    g3 = (left - g2.astype(F32)).astype(BF16)
    back = jnp.dot(low_first, g1, preferred_element_type=F32)
    back += jnp.dot(low_first, g2, preferred_element_type=F32)
    back += jnp.dot(low_first, g3, preferred_element_type=F32)
    coeff_out[...] = total + (total - back)
    coeff_copy_out = pltpu.make_async_copy(coeff_out, coeff_to, out_sem.at[1])
    coeff_copy_out.start()
    finish()
    for o in range(1, n_g * n_y):
        gram_a(o).wait_send()
        gram_c(o).wait_send()
    for o in range(1, n_x):
        gram_b(o).wait_send()

    def snap_sent(k, carry):
        for o in range(1, n_g):
            snap_copy(k, o).wait_send()
        return carry

    lax.fori_loop(0, ROUNDS, snap_sent, 0)
    adj_copy.wait()
    coeff_copy_out.wait()


def body(terminal, diffusion, velocity, material, rates, stoich, plan, basis):
    sm = pltpu.SMEM
    dma = pltpu.SemaphoreType.DMA
    v = pltpu.VMEM
    return pl.pallas_call(
        kernel,
        out_shape=(
            jax.ShapeDtypeStruct((SNAPS, MODES), F32),
            jax.ShapeDtypeStruct((SPEC, CX, CY, CZ), F32),
        ),
        in_specs=[pl.BlockSpec(memory_space=pl.ANY)] * 8,
        out_specs=(pl.BlockSpec(memory_space=pl.ANY),) * 2,
        scratch_shapes=[
            sm((SPEC,), F32),
            sm((MATS, 8), F32),
            sm((SPEC, 8), jnp.int32),
            sm((SNAPS,), jnp.int32),
            v((CX, CY, CZ), jnp.int32),
            v((SNAPS, MODES), F32),
            dma((7,)),
            dma((2,)),
            v((BASIS_ROWS, MODES), BF16),
            v((STEPS + 1, SPEC, CX, CY, CZ), F32),
            v((2, CX, CY, CZ), F32),
            v((2, 2, SPEC, 2, CY, CZ), F32),
            v((2, 2, SPEC, CX, 8, CZ), F32),
            v((2, 2, 8, CZ), F32),
            v((2, 6, 8, CZ), F32),
            v((2, 12, 8, CZ), F32),
            v((2, 2, 1, CY, CZ), F32),
            v((2, 2, CX, 8, CZ), F32),
            v((2, 2, CX, CY, CZ), F32),
            v((SPEC, 8, 24, 256), F32),
            v((SPEC, 6, 24, 256), F32),
            v((SPEC, 6, 24, 256), F32),
            v((6, 24, 256), F32),
            v((SPEC, 6, 24, 256), F32),
            v((SPEC, SPEC, 6, 24, 256), F32),
            v((MODES, MODES), F32),
            v((STEPS, 4, CX, CY, CZ), F32),
            v((2 * STEPS, MODES), F32),
            v((16, SNAPS, MODES), F32),
            v((8, SNAPS, MODES), F32),
            v((16, 16, MODES), F32),
            v((8, 16, MODES), F32),
            v((MODES, MODES), F32),
            dma((ROUNDS,)),
            dma((2, 18)),
            dma((2, 18)),
            dma((6,)),
            dma((6,)),
            dma((ROUNDS, 3)),
            dma((ROUNDS, 3)),
            dma((2, 16)),
            dma((2, 16)),
            dma((3, 16)),
            dma((3, 16)),
        ],
        compiler_params=pltpu.CompilerParams(
            collective_id=0, has_side_effects=True, vmem_limit_bytes=60 * 1024 * 1024
        ),
    )(
        terminal, diffusion, velocity, material, rates, stoich.T, plan,
        basis.reshape(BASIS_ROWS, MODES),
    )


def solution(mesh):
    return jax.shard_map(
        body,
        mesh=mesh,
        in_specs=(
            P(None, "gx", "gy", "grp"),
            P(),
            P("gx", "gy", "grp"),
            P("gx", "gy", "grp"),
            P(),
            P(),
            P(),
            P("grp", "gx", "gy", None, None),
        ),
        out_specs=(P(), P(None, "gx", "gy", "grp")),
        check_vma=False,
    )
```

```python
import jax
import jax.numpy as jnp
from jax import lax
from jax.experimental import pallas as pl
from jax.experimental.pallas import tpu as pltpu
from jax.sharding import PartitionSpec as P

SPEC = 4
MATS = 8
STEPS = 16
ROUNDS = STEPS // 2
SNAPS = 8
MODES = 256
CX, CY, CZ = 4, 16, 128
ROWS = CX * CY
BASIS_ROWS = ROWS * 512
PART = BASIS_ROWS // ROUNDS
MESH = pl.DeviceIdType.MESH
F32 = jnp.float32
BF16 = jnp.bfloat16

FACES = [(-1, 0, 0), (1, 0, 0), (0, -1, 0), (0, 1, 0), (0, 0, -1), (0, 0, 1)]
XZ = [(a, 0, b) for a in (-1, 1) for b in (-1, 1)]
XY = [(a, b, 0) for a in (-1, 1) for b in (-1, 1)]
YZ = [(0, a, b) for a in (-1, 1) for b in (-1, 1)]
DIRS = FACES + XZ + XY + YZ
ORDER = [6, 7, 8, 9, 10, 11, 12, 13, 0, 1, 14, 15, 16, 17, 4, 5, 2, 3]


def kernel(
    terminal_in, diffusion_in, velocity_in, material_in, rates_in, stoich_in, plan_in, basis,
    joined,
    diffusion, rates, stoich, plan, material, coeff_out, in_sem, out_sem, bv, st, fields, rx, ry, rz, pack, edge, cx, cy, cz, lam, mid,
    kc, vm, dm, rc, gram, got, proj, suma, sumb, gparts, gsums, gfull, gsplit,
    basis_sem, hs, hr, cs, cr, as_, ar, ss, sr, gs, gr,
):
    g = lax.axis_index("grp")
    x = lax.axis_index("gx")
    y = lax.axis_index("gy")
    n_g, n_x, n_y = 4, 8, 4

    def has(d):
        cond = None
        for step, at, count in ((d[0], x, n_x), (d[1], y, n_y), (d[2], g, n_g)):
            if step == 0:
                continue
            term = at > 0 if step < 0 else at < count - 1
            cond = term if cond is None else jnp.logical_and(cond, term)
        return cond

    def minus(d):
        return tuple(-v for v in d)

    def dev(d):
        return (g + d[2], x + d[0], y + d[1])

    sub = lax.broadcasted_iota(jnp.int32, (8, CZ), 0)
    lane = lax.broadcasted_iota(jnp.int32, (8, CZ), 1)
    odd_lane = lax.rem(lane, 2) == 1
    odd_sub = lax.rem(sub, 2) == 1

    def low(cond, most):
        return jnp.where(cond, most, 0)

    def high(cond, least, size):
        return jnp.where(cond, least, size)

    def basis_copy(c):
        rows = pl.ds(c * PART, PART)
        return pltpu.make_async_copy(basis.at[rows, :], bv.at[rows, :], basis_sem.at[c])

    inputs = [
        pltpu.make_async_copy(src, dst, in_sem.at[i]) for i, (src, dst) in enumerate((
            (terminal_in, st.at[0]), (velocity_in, fields.at[0]), (material_in, material),
            (diffusion_in, diffusion), (rates_in, rates), (stoich_in, stoich),
            (plan_in, plan)))
    ]
    for copy in inputs:
        copy.start()
    for c in range(ROUNDS):
        basis_copy(c).start()


    barrier = pltpu.get_barrier_semaphore()
    ga = g * n_y + y

    def group_a(o):
        q = lax.rem(ga + o, n_g * n_y)
        return q, (q // n_y, x, lax.rem(q, n_y))

    def group_b(o):
        q = lax.rem(x + o, n_x)
        return q, (g, q, y)

    count = jnp.int32(n_g * n_y - 1 + n_x - 1)
    for d in XZ + XY:
        cond = has(d)
        count = count + cond.astype(jnp.int32)

        @pl.when(cond)
        def _(d=d):
            pl.semaphore_signal(barrier, inc=1, device_id=dev(d), device_id_type=MESH)

    for o in (4, 3, 5, 2, 6, 1, 7):
        pl.semaphore_signal(barrier, inc=1, device_id=group_b(o)[1], device_id_type=MESH)
    for o in range(1, n_g * n_y):
        pl.semaphore_signal(barrier, inc=1, device_id=group_a(o)[1], device_id_type=MESH)

    lam[...] = jnp.zeros_like(lam)
    mid[...] = jnp.zeros_like(mid)
    gram[...] = jnp.zeros_like(gram)
    for copy in inputs:
        copy.wait()
    fields[1] = material[...].astype(F32)
    lam[:, 2:6, 0:16, 0:128] = st[0]
    pl.semaphore_wait(barrier, count)

    def halo_copy(i, k, par):
        d = DIRS[i]
        n = 2 * k
        if i < 2:
            src = st.at[n, :, pl.ds(0 if i == 0 else 2, 2)]
            dst = rx.at[par, i]
        elif i < 4:
            src = st.at[n, :, :, pl.ds(0 if i == 2 else 8, 8), :]
            dst = ry.at[par, i - 2]
        elif i < 6:
            src = pack.at[par, 5]
            dst = rz.at[par, i - 4]
        else:
            if i < 10:
                which = (i - 6) // 2
            elif i < 14:
                which = 2 + (i - 10) // 2
            else:
                which = 4
            src = pack.at[par, which]
            dst = edge.at[par, i - 6]
        return pltpu.make_async_remote_copy(
            src_ref=src, dst_ref=dst, send_sem=hs.at[par, i], recv_sem=hr.at[par, i],
            device_id=dev(d), device_id_type=MESH,
        )

    def pack_x_edges(k, par):
        n = 2 * k
        for side in (0, 1):
            plane = 0 if side == 0 else CX - 1
            acc = jnp.zeros((8, CZ), F32)
            rows = jnp.zeros((8, CZ), F32)
            for s in range(SPEC):
                t0 = st[n, s, plane, 0:8, :]
                t1 = st[n, s, plane, 8:16, :]
                for t, v in ((0, t0), (1, t1)):
                    i = 2 * (s * 2 + t)
                    hit = jnp.logical_or(lane == i, lane == (i - 1) % CZ)
                    acc = jnp.where(hit, pltpu.roll(v, i, 1) if i else v, acc)
                i = 2 * s
                both = jnp.where(sub < 4, t0, t1)
                hit = jnp.logical_or(sub == i, sub == (i - 1) % 8)
                rows = jnp.where(hit, pltpu.roll(both, i, 0) if i else both, rows)
            pack[par, side] = acc
            pack[par, 2 + side] = rows

    def pack_others(k, par):
        n = 2 * k
        acc = jnp.zeros((8, CZ), F32)
        face = jnp.zeros((8, CZ), F32)
        for s in range(SPEC):
            for p in range(CX):
                t0 = st[n, s, p, 0:8, :]
                t1 = st[n, s, p, 8:16, :]
                i = 2 * (s * CX + p)
                v = jnp.where(sub < 4, t0, t1)
                hit = jnp.logical_or(lane == i, lane == (i - 1) % CZ)
                acc = jnp.where(hit, pltpu.roll(v, i, 1) if i else v, acc)
                for t, v in ((0, t0), (1, t1)):
                    i = 4 * ((s * CX + p) * 2 + t)
                    place = lax.rem(lane + (CZ + 2 - i), CZ)
                    face = jnp.where(place < 4, pltpu.roll(v, i, 1) if i else v, face)
        pack[par, 4] = acc
        pack[par, 5] = face

    def send(i, k, par):
        @pl.when(has(DIRS[i]))
        def _():
            halo_copy(i, k, par).start()

    def start_halo(k, par):
        pack_x_edges(k, par)
        for i in ORDER[:10]:
            send(i, k, par)
        pack_others(k, par)
        for i in ORDER[10:]:
            send(i, k, par)

    def wait_halo(k, par, which):
        for i in which:

            @pl.when(has(minus(DIRS[i])))
            def _(i=i):
                halo_copy(i, k, par).wait_recv()

    def wait_sent(k, par):
        for i in ORDER:

            @pl.when(has(DIRS[i]))
            def _(i=i):
                halo_copy(i, k, par).wait_send()

    xm, xp = has((-1, 0, 0)), has((1, 0, 0))
    ym, yp = has((0, -1, 0)), has((0, 1, 0))
    zm, zp = has((0, 0, -1)), has((0, 0, 1))
    y_from_p = sub < low(yp, 4)
    y_from_m = sub >= high(ym, 4, 8)
    lane_full = lax.broadcasted_iota(jnp.int32, (CY, CZ), 1)
    z_from_p = lane_full < low(zp, 64)
    z_from_m = lane_full >= high(zm, 64, CZ)

    def flag(a, b):
        return jnp.logical_and(a, b)

    even_lane = jnp.logical_not(odd_lane)
    zero8 = jnp.zeros((8, CZ), F32)

    def unpack_yz(par):
        far = lax.rem(lane, 4) >= 2
        comb = jnp.where(
            flag(far, lane < low(zm, CZ)), rz[par, 1],
            jnp.where(flag(jnp.logical_not(far), lane < low(zp, CZ)), rz[par, 0], zero8))
        hi_m = flag(odd_lane, sub >= high(flag(ym, zm), 4, 8))
        hi_p = flag(even_lane, sub >= high(flag(ym, zp), 4, 8))
        lo_m = flag(odd_lane, sub < low(flag(yp, zm), 4))
        lo_p = flag(even_lane, sub < low(flag(yp, zp), 4))
        corner = jnp.where(hi_m, edge[par, 11], zero8)
        corner = jnp.where(hi_p, edge[par, 10], corner)
        corner = jnp.where(lo_m, edge[par, 9], corner)
        corner = jnp.where(lo_p, edge[par, 8], corner)
        for s in range(SPEC):
            for p in range(CX):
                lam[s, 2 + p, 16:24, 0:128] = jnp.where(
                    y_from_p, ry[par, 0, s, p], jnp.where(y_from_m, ry[par, 1, s, p], zero8))
                for t in range(2):
                    i = 4 * ((s * CX + p) * 2 + t)
                    tile = pltpu.roll(comb, (CZ - i) % CZ, 1) if i else comb
                    lam[s, 2 + p, t * 8:(t + 1) * 8, 128:256] = tile
                i = 2 * (s * CX + p)
                tile = pltpu.roll(corner, (CZ - i) % CZ, 1) if i else corner
                lam[s, 2 + p, 16:24, 128:256] = tile

    def unpack_x(par):
        for s in range(SPEC):
            lam[s, 0:2, 0:16, 0:128] = jnp.where(xm, rx[par, 1, s], 0.0)
            lam[s, 6:8, 0:16, 0:128] = jnp.where(xp, rx[par, 0, s], 0.0)
        for side, xh in ((1, xm), (0, xp)):
            at = 1 if side == 1 else 6
            base = side * 2
            comb = jnp.where(
                flag(odd_lane, lane < low(flag(xh, zm), CZ)), edge[par, base + 1],
                jnp.where(
                    flag(even_lane, lane < low(flag(xh, zp), CZ)), edge[par, base], zero8))
            base = 4 + side * 2
            rows = jnp.where(
                flag(odd_sub, sub < low(flag(xh, ym), 8)), edge[par, base + 1],
                jnp.where(
                    flag(jnp.logical_not(odd_sub), sub < low(flag(xh, yp), 8)),
                    edge[par, base], zero8))
            for s in range(SPEC):
                for t in range(2):
                    i = 2 * (s * 2 + t)
                    tile = pltpu.roll(comb, (CZ - i) % CZ, 1) if i else comb
                    lam[s, at, t * 8:(t + 1) * 8, 128:256] = tile
                i = 2 * s
                tile = pltpu.roll(rows, (8 - i) % 8, 0) if i else rows
                lam[s, at, 16:24, 0:128] = tile

    def coeff_copy(i):
        if i < 2:
            src = fields.at[:, pl.ds(0 if i == 0 else CX - 1, 1)]
            dst = cx.at[i]
        elif i < 4:
            src = fields.at[:, :, pl.ds(0 if i == 2 else 8, 8), :]
            dst = cy.at[i - 2]
        else:
            src = fields
            dst = cz.at[i - 4]
        return pltpu.make_async_remote_copy(
            src_ref=src, dst_ref=dst, send_sem=cs.at[i], recv_sem=cr.at[i],
            device_id=dev(DIRS[i]), device_id_type=MESH,
        )

    def snap_copy(k, o):
        q = lax.rem(g + o, n_g)
        return pltpu.make_async_remote_copy(
            src_ref=st.at[pl.ds(2 * k + 1, 2), q],
            dst_ref=got.at[pl.ds(2 * k, 2), g],
            send_sem=as_.at[k, o - 1], recv_sem=ar.at[k, o - 1],
            device_id=(q, x, y), device_id_type=MESH,
        )


    def coefficients(outer):
        for p in range(6):
            own = 1 <= p <= CX
            for r0, r1, l0, l1 in ((0, 16, 0, 128), (16, 24, 0, 128), (0, 16, 128, 256)):
                if not own and (r0, l0) != (0, 0):
                    continue
                if outer == (own and (r0, l0) == (0, 0)):
                    continue
                vals = []
                for f in range(2):
                    if not own:
                        side, ok = (1, xm) if p == 0 else (0, xp)
                        v = jnp.where(ok, cx[side, f, 0], 0.0)
                    elif (r0, l0) == (0, 0):
                        v = fields[f, p - 1]
                    elif r0 == 16:
                        v = jnp.where(y_from_p, cy[0, f, p - 1],
                                      jnp.where(y_from_m, cy[1, f, p - 1], 0.0))
                    else:
                        v = jnp.where(z_from_p, cz[0, f, p - 1],
                                      jnp.where(z_from_m, cz[1, f, p - 1], 0.0))
                    vals.append(v)
                vel, mat = vals
                if not own:
                    ok = xm if p == 0 else xp
                    inside = jnp.where(ok, 1.0, 0.0) * jnp.ones((16, 128), F32)
                elif (r0, l0) == (0, 0):
                    inside = jnp.ones((16, 128), F32)
                elif r0 == 16:
                    inside = jnp.where(jnp.logical_or(y_from_p, y_from_m), 1.0, 0.0)
                else:
                    inside = jnp.where(jnp.logical_or(z_from_p, z_from_m), 1.0, 0.0)
                looked = []
                for r in range(8):
                    v = jnp.full(mat.shape, rates[0, r], F32)
                    for m in range(1, MATS):
                        v = jnp.where(mat == float(m), rates[m, r], v)
                    looked.append(v * inside)
                vel = vel * inside
                vm[p, r0:r1, l0:l1] = vel
                for a in range(SPEC):
                    dm[a, p, r0:r1, l0:l1] = inside * diffusion[a]
                    for b in range(SPEC):
                        v = (looked[a] * stoich[b, a].astype(F32)
                             + looked[a + 4] * stoich[b, a + 4].astype(F32))
                        if a == b:
                            kc[a, p, r0:r1, l0:l1] = (
                                inside * (1.0 - 6.0 * diffusion[a]) - vel + v)
                        else:
                            rc[a, b, p, r0:r1, l0:l1] = v

    def advance(cs_, s, p, tile, dn, up, ys, zs):
        r0, r1, l0, l1 = tile
        box = (p, slice(r0, r1), slice(l0, l1))
        total = dm[(s,) + box] * (((dn + up) + ys) + zs)
        total = total + kc[(s,) + box] * cs_[s]
        total = total + vm[box] * up
        for b in range(SPEC):
            if b != s:
                total = total + rc[(s, b) + box] * cs_[b]
        return total

    own_tile = (0, 16, 0, 128)

    def first_step(planes):
        for p in planes:
            full = [lam[s, p + 1] for s in range(SPEC)]
            for s in range(SPEC):
                c = full[s]
                ya = pltpu.roll(c, 1, 0) + pltpu.roll(c, 23, 0)
                za = pltpu.roll(c, 1, 1) + pltpu.roll(c, 255, 1)
                tiles = [own_tile]
                if 1 <= p <= CX:
                    tiles += [(16, 24, 0, 128), (0, 16, 128, 256)]
                for t in tiles:
                    r0, r1, l0, l1 = t
                    mid[s, p, r0:r1, l0:l1] = advance(
                        [v[r0:r1, l0:l1] for v in full], s, p, t,
                        lam[s, p, r0:r1, l0:l1], lam[s, p + 2, r0:r1, l0:l1],
                        ya[r0:r1, l0:l1], za[r0:r1, l0:l1])

    def second_step(n):
        for p in range(1, 1 + CX):
            own = [mid[s, p, 0:16, 0:128] for s in range(SPEC)]
            for s in range(SPEC):
                col = mid[s, p, :, 0:128]
                ya = (pltpu.roll(col, 1, 0) + pltpu.roll(col, 23, 0))[0:16]
                row = mid[s, p, 0:16, :]
                za = (pltpu.roll(row, 1, 1) + pltpu.roll(row, 255, 1))[:, 0:128]
                new = advance(own, s, p, own_tile, mid[s, p - 1, 0:16, 0:128],
                              mid[s, p + 1, 0:16, 0:128], ya, za)
                st[n + 1, s, p - 1] = own[s]
                st[n + 2, s, p - 1] = new
                lam[s, p + 1, 0:16, 0:128] = new

    block_rows = 1024

    def gram_blocks(start, count):
        def one(c, carry):
            at = pl.multiple_of((start + c) * block_rows, block_rows)
            block = bv[pl.ds(at, block_rows), :]
            gram[...] += lax.dot_general(
                block, block, (((0,), (0,)), ((), ())), preferred_element_type=F32)
            return carry

        lax.fori_loop(0, count, one, 0)

    slab = MODES // (n_g * n_y)

    def slab_of(q):
        return pl.ds(pl.multiple_of(q * slab, slab), slab)

    def gram_a(o):
        q, where = group_a(o)
        return pltpu.make_async_remote_copy(
            src_ref=gram.at[slab_of(q), :], dst_ref=gparts.at[ga],
            send_sem=gs.at[0, o], recv_sem=gr.at[0, o], device_id=where, device_id_type=MESH)

    def gram_b(o):
        q, where = group_b(o)
        return pltpu.make_async_remote_copy(
            src_ref=gsums.at[x], dst_ref=gsums.at[x],
            send_sem=gs.at[1, o], recv_sem=gr.at[1, o], device_id=where, device_id_type=MESH)

    def gram_c(o):
        q, where = group_a(o)
        return pltpu.make_async_remote_copy(
            src_ref=gfull.at[slab_of(ga), :], dst_ref=gfull.at[slab_of(ga), :],
            send_sem=gs.at[2, o], recv_sem=gr.at[2, o], device_id=where, device_id_type=MESH)

    def gram_start():
        gparts[ga] = gram[slab_of(ga), :]
        for o in range(1, n_g * n_y):
            gram_a(o).start()

    def gram_middle():
        for o in range(1, n_g * n_y):
            gram_a(o).wait_recv()
        total = gparts[0]
        for q in range(1, n_g * n_y):
            total = total + gparts[q]
        gsums[x] = total
        for o in range(1, n_x):
            gram_b(o).start()

    def gram_last():
        for o in range(1, n_x):
            gram_b(o).wait_recv()
        total = gsums[0]
        for q in range(1, n_x):
            total = total + gsums[q]
        gfull[slab_of(ga), :] = total
        for o in range(1, n_g * n_y):
            gram_c(o).start()

    start_halo(0, 0)
    for i in range(6):

        @pl.when(has(DIRS[i]))
        def _(i=i):
            coeff_copy(i).start()

    coefficients(False)
    for c in range(2):
        basis_copy(c).wait()
    gram_blocks(0, 8)
    for i in range(6):

        @pl.when(has(minus(DIRS[i])))
        def _(i=i):
            coeff_copy(i).wait_recv()

    coefficients(True)

    def round_(k, carry):
        par = lax.rem(k, 2)

        @pl.when(k > 0)
        def _():
            start_halo(k, par)
            for o in range(1, n_g):
                snap_copy(k - 1, o).start()

        @pl.when(k == 1)
        def _():
            for c in range(2, ROUNDS):
                basis_copy(c).wait()

        @pl.when(jnp.logical_and(k > 0, k < 5))
        def _():
            gram_blocks(2 + 6 * k, 6)

        @pl.when(k == 5)
        def _():
            gram_start()

        @pl.when(k == 6)
        def _():
            gram_middle()

        @pl.when(k == 7)
        def _():
            gram_last()

        wait_halo(k, par, ORDER[10:])
        unpack_yz(par)
        first_step((2, 3))
        wait_halo(k, par, ORDER[:10])
        unpack_x(par)
        first_step((0, 1, 4, 5))
        second_step(2 * k)
        wait_sent(k, par)
        got[pl.ds(2 * k, 2), g] = st[pl.ds(2 * k + 1, 2), g]
        return carry

    lax.fori_loop(0, ROUNDS, round_, 0)
    for o in (2, 1, 3):
        snap_copy(ROUNDS - 1, o).start()
    adj_copy = pltpu.make_async_copy(
        st.at[STEPS], joined.at[pl.ds(0, SPEC)], out_sem.at[0])
    adj_copy.start()
    for i in range(6):

        @pl.when(has(DIRS[i]))
        def _(i=i):
            coeff_copy(i).wait_send()

    flat = got.reshape(STEPS * 4 * ROWS, CZ)
    proj[...] = jnp.zeros_like(proj)
    unroll = 16

    def project(zq):
        def one(c, total):
            vals, blocks = [], []
            for u in range(unroll):
                at = c * unroll + u
                vals.append(flat[pl.ds(zq * ROWS + at, STEPS, stride=4 * ROWS), :])
                blocks.append(
                    bv[pl.ds(pl.multiple_of(at * 512 + zq * CZ, CZ), CZ), :])
            a = jnp.concatenate(vals, axis=1)
            hi = a.astype(BF16)
            lo = (a - hi.astype(F32)).astype(BF16)
            both = jnp.concatenate([hi, lo], axis=0)
            return total + jnp.dot(
                both, jnp.concatenate(blocks, axis=0), preferred_element_type=F32)

        proj[...] = lax.fori_loop(0, ROWS // unroll, one, proj[...])

    project(g)
    for o in (1, 3, 2):
        def snap_wait(k, carry, o=o):
            snap_copy(k, o).wait_recv()
            return carry

        lax.fori_loop(0, ROUNDS, snap_wait, 0)
        project(lax.rem(g + n_g - o, n_g))

    slot = lax.broadcasted_iota(jnp.int32, (SNAPS, MODES), 0)
    step_of = jnp.zeros((SNAPS, MODES), jnp.int32)
    for j in range(SNAPS):
        step_of = jnp.where(slot == j, plan[j], step_of)
    first = jnp.zeros((SNAPS, MODES), F32)
    for n in range(STEPS):
        row = proj[n:n + 1, :] + proj[STEPS + n:STEPS + n + 1, :]
        first = jnp.where(step_of == n, jnp.broadcast_to(row, first.shape), first)

    def all_sum(value):
        suma[ga] = value

        def a_copy(o):
            q, where = group_a(o)
            return pltpu.make_async_remote_copy(
                src_ref=suma.at[ga], dst_ref=suma.at[ga],
                send_sem=ss.at[0, o], recv_sem=sr.at[0, o],
                device_id=where, device_id_type=MESH)

        def b_copy(o):
            q, where = group_b(o)
            return pltpu.make_async_remote_copy(
                src_ref=sumb.at[x], dst_ref=sumb.at[x],
                send_sem=ss.at[1, o], recv_sem=sr.at[1, o],
                device_id=where, device_id_type=MESH)

        for o in range(1, n_g * n_y):
            a_copy(o).start()
        for o in range(1, n_g * n_y):
            gram_c(o).wait_recv()
        gm = gfull[...]
        g1 = gm.astype(BF16)
        left = gm - g1.astype(F32)
        g2 = left.astype(BF16)
        gsplit[0] = g1
        gsplit[1] = g2
        gsplit[2] = (left - g2.astype(F32)).astype(BF16)
        for o in range(1, n_g * n_y):
            a_copy(o).wait_recv()
        total = suma[0]
        for q in range(1, n_g * n_y):
            total = total + suma[q]
        sumb[x] = total
        for o in range(1, n_x):
            b_copy(o).start()
        for o in range(1, n_x):
            b_copy(o).wait_recv()
        total = sumb[0]
        for q in range(1, n_x):
            total = total + sumb[q]

        def finish():
            for o in range(1, n_g * n_y):
                a_copy(o).wait_send()
            for o in range(1, n_x):
                b_copy(o).wait_send()

        return total, finish

    total, finish = all_sum(first)
    low_first = total.astype(BF16)
    back = jnp.dot(low_first, gsplit[0], preferred_element_type=F32)
    back += jnp.dot(low_first, gsplit[1], preferred_element_type=F32)
    back += jnp.dot(low_first, gsplit[2], preferred_element_type=F32)
    result = total + (total - back)
    coeff_out[0:SNAPS, :] = result[:, 0:CZ]
    coeff_out[SNAPS:2 * SNAPS, :] = result[:, CZ:MODES]
    coeff_copy_out = pltpu.make_async_copy(coeff_out, joined.at[SPEC, 0], out_sem.at[1])
    coeff_copy_out.start()
    finish()
    for o in range(1, n_g * n_y):
        gram_a(o).wait_send()
        gram_c(o).wait_send()
    for o in range(1, n_x):
        gram_b(o).wait_send()

    def snap_sent(k, carry):
        for o in range(1, n_g):
            snap_copy(k, o).wait_send()
        return carry

    lax.fori_loop(0, ROUNDS, snap_sent, 0)
    adj_copy.wait()
    coeff_copy_out.wait()


def divide(joined, coeff_to, adj_to, field, coeff, sem):
    lead = pltpu.make_async_copy(joined.at[pl.ds(0, SPEC)], field, sem.at[0])
    tail = pltpu.make_async_copy(joined.at[SPEC, 0], coeff, sem.at[1])
    lead.start()
    tail.start()
    tail.wait()
    halves = [
        pltpu.make_async_copy(
            coeff.at[pl.ds(h * SNAPS, SNAPS), :], coeff_to.at[:, pl.ds(h * CZ, CZ)],
            sem.at[2 + h])
        for h in range(2)
    ]
    for half in halves:
        half.start()
    lead.wait()
    last = pltpu.make_async_copy(field, adj_to, sem.at[4])
    last.start()
    for half in halves:
        half.wait()
    last.wait()


def body(terminal, diffusion, velocity, material, rates, stoich, plan, basis):
    sm = pltpu.SMEM
    dma = pltpu.SemaphoreType.DMA
    v = pltpu.VMEM
    joined = pl.pallas_call(
        kernel,
        out_shape=jax.ShapeDtypeStruct((SPEC + 1, CX, CY, CZ), F32),
        in_specs=[pl.BlockSpec(memory_space=pl.ANY)] * 8,
        out_specs=pl.BlockSpec(memory_space=pl.ANY),
        scratch_shapes=[
            sm((SPEC,), F32),
            sm((MATS, 8), F32),
            sm((SPEC, 8), jnp.int32),
            sm((SNAPS,), jnp.int32),
            v((CX, CY, CZ), jnp.int32),
            v((CY, CZ), F32),
            dma((7,)),
            dma((2,)),
            v((BASIS_ROWS, MODES), BF16),
            v((STEPS + 1, SPEC, CX, CY, CZ), F32),
            v((2, CX, CY, CZ), F32),
            v((2, 2, SPEC, 2, CY, CZ), F32),
            v((2, 2, SPEC, CX, 8, CZ), F32),
            v((2, 2, 8, CZ), F32),
            v((2, 6, 8, CZ), F32),
            v((2, 12, 8, CZ), F32),
            v((2, 2, 1, CY, CZ), F32),
            v((2, 2, CX, 8, CZ), F32),
            v((2, 2, CX, CY, CZ), F32),
            v((SPEC, 8, 24, 256), F32),
            v((SPEC, 6, 24, 256), F32),
            v((SPEC, 6, 24, 256), F32),
            v((6, 24, 256), F32),
            v((SPEC, 6, 24, 256), F32),
            v((SPEC, SPEC, 6, 24, 256), F32),
            v((MODES, MODES), F32),
            v((STEPS, 4, CX, CY, CZ), F32),
            v((2 * STEPS, MODES), F32),
            v((16, SNAPS, MODES), F32),
            v((8, SNAPS, MODES), F32),
            v((16, 16, MODES), F32),
            v((8, 16, MODES), F32),
            v((MODES, MODES), F32),
            v((3, MODES, MODES), BF16),
            dma((ROUNDS,)),
            dma((2, 18)),
            dma((2, 18)),
            dma((6,)),
            dma((6,)),
            dma((ROUNDS, 3)),
            dma((ROUNDS, 3)),
            dma((2, 16)),
            dma((2, 16)),
            dma((3, 16)),
            dma((3, 16)),
        ],
        compiler_params=pltpu.CompilerParams(
            collective_id=0, has_side_effects=True, vmem_limit_bytes=60 * 1024 * 1024
        ),
    )(
        terminal, diffusion, velocity, material, rates, stoich.T, plan,
        basis.reshape(BASIS_ROWS, MODES),
    )
    return pl.pallas_call(
        divide,
        out_shape=(
            jax.ShapeDtypeStruct((SNAPS, MODES), F32),
            jax.ShapeDtypeStruct((SPEC, CX, CY, CZ), F32),
        ),
        in_specs=[pl.BlockSpec(memory_space=pl.ANY)],
        out_specs=(pl.BlockSpec(memory_space=pl.ANY),) * 2,
        scratch_shapes=[v((SPEC, CX, CY, CZ), F32), v((CY, CZ), F32), dma((5,))],
        compiler_params=pltpu.CompilerParams(vmem_limit_bytes=60 * 1024 * 1024),
    )(joined)


def solution(mesh):
    return jax.shard_map(
        body,
        mesh=mesh,
        in_specs=(
            P(None, "gx", "gy", "grp"),
            P(),
            P("gx", "gy", "grp"),
            P("gx", "gy", "grp"),
            P(),
            P(),
            P(),
            P("grp", "gx", "gy", None, None),
        ),
        out_specs=(P(), P(None, "gx", "gy", "grp")),
        check_vma=False,
    )
```

```python
import jax
import jax.numpy as jnp
from jax import lax
from jax.experimental import pallas as pl
from jax.experimental.pallas import tpu as pltpu
from jax.sharding import PartitionSpec as P

SPEC = 4
MATS = 8
STEPS = 16
ROUNDS = STEPS // 2
SNAPS = 8
MODES = 256
CX, CY, CZ = 4, 16, 128
ROWS = CX * CY
BASIS_ROWS = ROWS * 512
PART = BASIS_ROWS // ROUNDS
MESH = pl.DeviceIdType.MESH
F32 = jnp.float32
BF16 = jnp.bfloat16

FACES = [(-1, 0, 0), (1, 0, 0), (0, -1, 0), (0, 1, 0), (0, 0, -1), (0, 0, 1)]
XZ = [(a, 0, b) for a in (-1, 1) for b in (-1, 1)]
XY = [(a, b, 0) for a in (-1, 1) for b in (-1, 1)]
YZ = [(0, a, b) for a in (-1, 1) for b in (-1, 1)]
DIRS = FACES + XZ + XY + YZ
ORDER = [6, 7, 8, 9, 10, 11, 12, 13, 0, 1, 14, 15, 16, 17, 4, 5, 2, 3]


def kernel(
    terminal_in, diffusion_in, velocity_in, material_in, rates_in, stoich_in, plan_in, basis,
    joined,
    diffusion, rates, stoich, plan, material, coeff_out, in_sem, out_sem, bv, st, fields, rx, ry, rz, ypack, pack, edge, cx, cy, cz, lam, mid,
    kc, vm, dm, rc, gram, got, proj, suma, sumb, gparts, gsums, gfull, gsplit,
    basis_sem, hs, hr, cs, cr, as_, ar, ss, sr, gs, gr,
):
    g = lax.axis_index("grp")
    x = lax.axis_index("gx")
    y = lax.axis_index("gy")
    n_g, n_x, n_y = 4, 8, 4

    def has(d):
        cond = None
        for step, at, count in ((d[0], x, n_x), (d[1], y, n_y), (d[2], g, n_g)):
            if step == 0:
                continue
            term = at > 0 if step < 0 else at < count - 1
            cond = term if cond is None else jnp.logical_and(cond, term)
        return cond

    def minus(d):
        return tuple(-v for v in d)

    def dev(d):
        return (g + d[2], x + d[0], y + d[1])

    sub = lax.broadcasted_iota(jnp.int32, (8, CZ), 0)
    lane = lax.broadcasted_iota(jnp.int32, (8, CZ), 1)
    odd_lane = lax.rem(lane, 2) == 1
    odd_sub = lax.rem(sub, 2) == 1

    def low(cond, most):
        return jnp.where(cond, most, 0)

    def high(cond, least, size):
        return jnp.where(cond, least, size)

    def basis_copy(c):
        rows = pl.ds(c * PART, PART)
        return pltpu.make_async_copy(basis.at[rows, :], bv.at[rows, :], basis_sem.at[c])

    inputs = [
        pltpu.make_async_copy(src, dst, in_sem.at[i]) for i, (src, dst) in enumerate((
            (terminal_in, st.at[0]), (velocity_in, fields.at[0]), (material_in, material),
            (diffusion_in, diffusion), (rates_in, rates), (stoich_in, stoich),
            (plan_in, plan)))
    ]
    for copy in inputs:
        copy.start()
    for c in range(ROUNDS):
        basis_copy(c).start()


    barrier = pltpu.get_barrier_semaphore()
    ga = g * n_y + y

    def group_a(o):
        q = lax.rem(ga + o, n_g * n_y)
        return q, (q // n_y, x, lax.rem(q, n_y))

    def group_b(o):
        q = lax.rem(x + o, n_x)
        return q, (g, q, y)

    count = jnp.int32(n_g * n_y - 1 + n_x - 1)
    for d in XZ + XY:
        cond = has(d)
        count = count + cond.astype(jnp.int32)

        @pl.when(cond)
        def _(d=d):
            pl.semaphore_signal(barrier, inc=1, device_id=dev(d), device_id_type=MESH)

    for o in (4, 3, 5, 2, 6, 1, 7):
        pl.semaphore_signal(barrier, inc=1, device_id=group_b(o)[1], device_id_type=MESH)
    for o in range(1, n_g * n_y):
        pl.semaphore_signal(barrier, inc=1, device_id=group_a(o)[1], device_id_type=MESH)

    lam[...] = jnp.zeros_like(lam)
    mid[...] = jnp.zeros_like(mid)
    gram[...] = jnp.zeros_like(gram)
    for copy in inputs:
        copy.wait()
    fields[1] = material[...].astype(F32)
    lam[:, 2:6, 0:16, 0:128] = st[0]
    pl.semaphore_wait(barrier, count)

    def halo_copy(i, k, par):
        d = DIRS[i]
        n = 2 * k
        if i < 2:
            src = st.at[n, :, pl.ds(0 if i == 0 else 2, 2)]
            dst = rx.at[par, i]
        elif i < 4:
            src = ypack.at[par, i - 2]
            dst = ry.at[par, i - 2]
        elif i < 6:
            src = pack.at[par, 5]
            dst = rz.at[par, i - 4]
        else:
            if i < 10:
                which = (i - 6) // 2
            elif i < 14:
                which = 2 + (i - 10) // 2
            else:
                which = 4
            src = pack.at[par, which]
            dst = edge.at[par, i - 6]
        return pltpu.make_async_remote_copy(
            src_ref=src, dst_ref=dst, send_sem=hs.at[par, i], recv_sem=hr.at[par, i],
            device_id=dev(d), device_id_type=MESH,
        )

    def pack_x_edges(k, par):
        n = 2 * k
        for side in (0, 1):
            plane = 0 if side == 0 else CX - 1
            acc = jnp.zeros((8, CZ), F32)
            rows = jnp.zeros((8, CZ), F32)
            for s in range(SPEC):
                t0 = st[n, s, plane, 0:8, :]
                t1 = st[n, s, plane, 8:16, :]
                for t, v in ((0, t0), (1, t1)):
                    i = 2 * (s * 2 + t)
                    hit = jnp.logical_or(lane == i, lane == (i - 1) % CZ)
                    acc = jnp.where(hit, pltpu.roll(v, i, 1) if i else v, acc)
                i = 2 * s
                both = jnp.where(sub < 4, t0, t1)
                hit = jnp.logical_or(sub == i, sub == (i - 1) % 8)
                rows = jnp.where(hit, pltpu.roll(both, i, 0) if i else both, rows)
            pack[par, side] = acc
            pack[par, 2 + side] = rows

    def pack_others(k, par):
        n = 2 * k
        acc = jnp.zeros((8, CZ), F32)
        face = jnp.zeros((8, CZ), F32)
        for s in range(SPEC):
            for p in range(CX):
                t0 = st[n, s, p, 0:8, :]
                t1 = st[n, s, p, 8:16, :]
                i = 2 * (s * CX + p)
                v = jnp.where(sub < 4, t0, t1)
                hit = jnp.logical_or(lane == i, lane == (i - 1) % CZ)
                acc = jnp.where(hit, pltpu.roll(v, i, 1) if i else v, acc)
                for t, v in ((0, t0), (1, t1)):
                    i = 4 * ((s * CX + p) * 2 + t)
                    place = lax.rem(lane + (CZ + 2 - i), CZ)
                    face = jnp.where(place < 4, pltpu.roll(v, i, 1) if i else v, face)
        pack[par, 4] = acc
        pack[par, 5] = face
        for s in range(SPEC):
            for h in range(2):
                a, b = 2 * h, 2 * h + 1
                ypack[par, 0, s, h] = jnp.where(
                    sub < 4, st[n, s, a, 0:8, :], pltpu.roll(st[n, s, b, 0:8, :], 4, 0))
                ypack[par, 1, s, h] = jnp.where(
                    sub >= 4, st[n, s, a, 8:16, :], pltpu.roll(st[n, s, b, 8:16, :], 4, 0))

    def send(i, k, par):
        @pl.when(has(DIRS[i]))
        def _():
            halo_copy(i, k, par).start()

    def start_halo(k, par):
        pack_x_edges(k, par)
        for i in ORDER[:10]:
            send(i, k, par)
        pack_others(k, par)
        for i in ORDER[10:]:
            send(i, k, par)

    def wait_halo(k, par, which):
        for i in which:

            @pl.when(has(minus(DIRS[i])))
            def _(i=i):
                halo_copy(i, k, par).wait_recv()

    def wait_sent(k, par):
        for i in ORDER:

            @pl.when(has(DIRS[i]))
            def _(i=i):
                halo_copy(i, k, par).wait_send()

    xm, xp = has((-1, 0, 0)), has((1, 0, 0))
    ym, yp = has((0, -1, 0)), has((0, 1, 0))
    zm, zp = has((0, 0, -1)), has((0, 0, 1))
    y_from_p = sub < low(yp, 4)
    y_from_m = sub >= high(ym, 4, 8)
    lane_full = lax.broadcasted_iota(jnp.int32, (CY, CZ), 1)
    z_from_p = lane_full < low(zp, 64)
    z_from_m = lane_full >= high(zm, 64, CZ)

    def flag(a, b):
        return jnp.logical_and(a, b)

    even_lane = jnp.logical_not(odd_lane)
    zero8 = jnp.zeros((8, CZ), F32)

    def unpack_yz(par):
        far = lax.rem(lane, 4) >= 2
        comb = jnp.where(
            flag(far, lane < low(zm, CZ)), rz[par, 1],
            jnp.where(flag(jnp.logical_not(far), lane < low(zp, CZ)), rz[par, 0], zero8))
        hi_m = flag(odd_lane, sub >= high(flag(ym, zm), 4, 8))
        hi_p = flag(even_lane, sub >= high(flag(ym, zp), 4, 8))
        lo_m = flag(odd_lane, sub < low(flag(yp, zm), 4))
        lo_p = flag(even_lane, sub < low(flag(yp, zp), 4))
        corner = jnp.where(hi_m, edge[par, 11], zero8)
        corner = jnp.where(hi_p, edge[par, 10], corner)
        corner = jnp.where(lo_m, edge[par, 9], corner)
        corner = jnp.where(lo_p, edge[par, 8], corner)
        for s in range(SPEC):
            for p in range(CX):
                t0, t1 = ry[par, 0, s, p // 2], ry[par, 1, s, p // 2]
                if p % 2:
                    t0, t1 = pltpu.roll(t0, 4, 0), pltpu.roll(t1, 4, 0)
                lam[s, 2 + p, 16:24, 0:128] = jnp.where(
                    y_from_p, t0, jnp.where(y_from_m, t1, zero8))
                for t in range(2):
                    i = 4 * ((s * CX + p) * 2 + t)
                    tile = pltpu.roll(comb, (CZ - i) % CZ, 1) if i else comb
                    lam[s, 2 + p, t * 8:(t + 1) * 8, 128:256] = tile
                i = 2 * (s * CX + p)
                tile = pltpu.roll(corner, (CZ - i) % CZ, 1) if i else corner
                lam[s, 2 + p, 16:24, 128:256] = tile

    def unpack_x(par):
        for s in range(SPEC):
            lam[s, 0:2, 0:16, 0:128] = jnp.where(xm, rx[par, 1, s], 0.0)
            lam[s, 6:8, 0:16, 0:128] = jnp.where(xp, rx[par, 0, s], 0.0)
        for side, xh in ((1, xm), (0, xp)):
            at = 1 if side == 1 else 6
            base = side * 2
            comb = jnp.where(
                flag(odd_lane, lane < low(flag(xh, zm), CZ)), edge[par, base + 1],
                jnp.where(
                    flag(even_lane, lane < low(flag(xh, zp), CZ)), edge[par, base], zero8))
            base = 4 + side * 2
            rows = jnp.where(
                flag(odd_sub, sub < low(flag(xh, ym), 8)), edge[par, base + 1],
                jnp.where(
                    flag(jnp.logical_not(odd_sub), sub < low(flag(xh, yp), 8)),
                    edge[par, base], zero8))
            for s in range(SPEC):
                for t in range(2):
                    i = 2 * (s * 2 + t)
                    tile = pltpu.roll(comb, (CZ - i) % CZ, 1) if i else comb
                    lam[s, at, t * 8:(t + 1) * 8, 128:256] = tile
                i = 2 * s
                tile = pltpu.roll(rows, (8 - i) % 8, 0) if i else rows
                lam[s, at, 16:24, 0:128] = tile

    def coeff_copy(i):
        if i < 2:
            src = fields.at[:, pl.ds(0 if i == 0 else CX - 1, 1)]
            dst = cx.at[i]
        elif i < 4:
            src = fields.at[:, :, pl.ds(0 if i == 2 else 8, 8), :]
            dst = cy.at[i - 2]
        else:
            src = fields
            dst = cz.at[i - 4]
        return pltpu.make_async_remote_copy(
            src_ref=src, dst_ref=dst, send_sem=cs.at[i], recv_sem=cr.at[i],
            device_id=dev(DIRS[i]), device_id_type=MESH,
        )

    def snap_copy(k, o):
        q = lax.rem(g + o, n_g)
        return pltpu.make_async_remote_copy(
            src_ref=st.at[pl.ds(2 * k + 1, 2), q],
            dst_ref=got.at[pl.ds(2 * k, 2), g],
            send_sem=as_.at[k, o - 1], recv_sem=ar.at[k, o - 1],
            device_id=(q, x, y), device_id_type=MESH,
        )


    def coefficients(outer):
        for p in range(6):
            own = 1 <= p <= CX
            for r0, r1, l0, l1 in ((0, 16, 0, 128), (16, 24, 0, 128), (0, 16, 128, 256)):
                if not own and (r0, l0) != (0, 0):
                    continue
                if outer == (own and (r0, l0) == (0, 0)):
                    continue
                vals = []
                for f in range(2):
                    if not own:
                        side, ok = (1, xm) if p == 0 else (0, xp)
                        v = jnp.where(ok, cx[side, f, 0], 0.0)
                    elif (r0, l0) == (0, 0):
                        v = fields[f, p - 1]
                    elif r0 == 16:
                        v = jnp.where(y_from_p, cy[0, f, p - 1],
                                      jnp.where(y_from_m, cy[1, f, p - 1], 0.0))
                    else:
                        v = jnp.where(z_from_p, cz[0, f, p - 1],
                                      jnp.where(z_from_m, cz[1, f, p - 1], 0.0))
                    vals.append(v)
                vel, mat = vals
                if not own:
                    ok = xm if p == 0 else xp
                    inside = jnp.where(ok, 1.0, 0.0) * jnp.ones((16, 128), F32)
                elif (r0, l0) == (0, 0):
                    inside = jnp.ones((16, 128), F32)
                elif r0 == 16:
                    inside = jnp.where(jnp.logical_or(y_from_p, y_from_m), 1.0, 0.0)
                else:
                    inside = jnp.where(jnp.logical_or(z_from_p, z_from_m), 1.0, 0.0)
                looked = []
                for r in range(8):
                    v = jnp.full(mat.shape, rates[0, r], F32)
                    for m in range(1, MATS):
                        v = jnp.where(mat == float(m), rates[m, r], v)
                    looked.append(v * inside)
                vel = vel * inside
                vm[p, r0:r1, l0:l1] = vel
                for a in range(SPEC):
                    dm[a, p, r0:r1, l0:l1] = inside * diffusion[a]
                    for b in range(SPEC):
                        v = (looked[a] * stoich[b, a].astype(F32)
                             + looked[a + 4] * stoich[b, a + 4].astype(F32))
                        if a == b:
                            kc[a, p, r0:r1, l0:l1] = (
                                inside * (1.0 - 6.0 * diffusion[a]) - vel + v)
                        else:
                            rc[a, b, p, r0:r1, l0:l1] = v

    def advance(cs_, s, p, tile, dn, up, ys, zs):
        r0, r1, l0, l1 = tile
        box = (p, slice(r0, r1), slice(l0, l1))
        total = dm[(s,) + box] * (((dn + up) + ys) + zs)
        total = total + kc[(s,) + box] * cs_[s]
        total = total + vm[box] * up
        for b in range(SPEC):
            if b != s:
                total = total + rc[(s, b) + box] * cs_[b]
        return total

    own_tile = (0, 16, 0, 128)

    def first_step(planes):
        for p in planes:
            full = [lam[s, p + 1] for s in range(SPEC)]
            for s in range(SPEC):
                c = full[s]
                ya = pltpu.roll(c, 1, 0) + pltpu.roll(c, 23, 0)
                za = pltpu.roll(c, 1, 1) + pltpu.roll(c, 255, 1)
                tiles = [own_tile]
                if 1 <= p <= CX:
                    tiles += [(16, 24, 0, 128), (0, 16, 128, 256)]
                for t in tiles:
                    r0, r1, l0, l1 = t
                    mid[s, p, r0:r1, l0:l1] = advance(
                        [v[r0:r1, l0:l1] for v in full], s, p, t,
                        lam[s, p, r0:r1, l0:l1], lam[s, p + 2, r0:r1, l0:l1],
                        ya[r0:r1, l0:l1], za[r0:r1, l0:l1])

    def second_step(n):
        for p in range(1, 1 + CX):
            own = [mid[s, p, 0:16, 0:128] for s in range(SPEC)]
            for s in range(SPEC):
                col = mid[s, p, :, 0:128]
                ya = (pltpu.roll(col, 1, 0) + pltpu.roll(col, 23, 0))[0:16]
                row = mid[s, p, 0:16, :]
                za = (pltpu.roll(row, 1, 1) + pltpu.roll(row, 255, 1))[:, 0:128]
                new = advance(own, s, p, own_tile, mid[s, p - 1, 0:16, 0:128],
                              mid[s, p + 1, 0:16, 0:128], ya, za)
                st[n + 1, s, p - 1] = own[s]
                st[n + 2, s, p - 1] = new
                lam[s, p + 1, 0:16, 0:128] = new

    block_rows = 1024

    def gram_blocks(start, count):
        def one(c, carry):
            at = pl.multiple_of((start + c) * block_rows, block_rows)
            block = bv[pl.ds(at, block_rows), :]
            gram[...] += lax.dot_general(
                block, block, (((0,), (0,)), ((), ())), preferred_element_type=F32)
            return carry

        lax.fori_loop(0, count, one, 0)

    slab = MODES // (n_g * n_y)

    def slab_of(q):
        return pl.ds(pl.multiple_of(q * slab, slab), slab)

    def gram_a(o):
        q, where = group_a(o)
        return pltpu.make_async_remote_copy(
            src_ref=gram.at[slab_of(q), :], dst_ref=gparts.at[ga],
            send_sem=gs.at[0, o], recv_sem=gr.at[0, o], device_id=where, device_id_type=MESH)

    def gram_b(o):
        q, where = group_b(o)
        return pltpu.make_async_remote_copy(
            src_ref=gsums.at[x], dst_ref=gsums.at[x],
            send_sem=gs.at[1, o], recv_sem=gr.at[1, o], device_id=where, device_id_type=MESH)

    def gram_c(o):
        q, where = group_a(o)
        return pltpu.make_async_remote_copy(
            src_ref=gfull.at[slab_of(ga), :], dst_ref=gfull.at[slab_of(ga), :],
            send_sem=gs.at[2, o], recv_sem=gr.at[2, o], device_id=where, device_id_type=MESH)

    def gram_start():
        gparts[ga] = gram[slab_of(ga), :]
        for o in range(1, n_g * n_y):
            gram_a(o).start()

    def gram_middle():
        for o in range(1, n_g * n_y):
            gram_a(o).wait_recv()
        total = gparts[0]
        for q in range(1, n_g * n_y):
            total = total + gparts[q]
        gsums[x] = total
        for o in range(1, n_x):
            gram_b(o).start()

    def gram_last():
        for o in range(1, n_x):
            gram_b(o).wait_recv()
        total = gsums[0]
        for q in range(1, n_x):
            total = total + gsums[q]
        gfull[slab_of(ga), :] = total
        for o in range(1, n_g * n_y):
            gram_c(o).start()

    start_halo(0, 0)
    for i in range(6):

        @pl.when(has(DIRS[i]))
        def _(i=i):
            coeff_copy(i).start()

    coefficients(False)
    for c in range(2):
        basis_copy(c).wait()
    gram_blocks(0, 8)
    for i in range(6):

        @pl.when(has(minus(DIRS[i])))
        def _(i=i):
            coeff_copy(i).wait_recv()

    coefficients(True)

    def round_(k, carry):
        par = lax.rem(k, 2)

        @pl.when(k > 0)
        def _():
            start_halo(k, par)
            for o in range(1, n_g):
                snap_copy(k - 1, o).start()

        @pl.when(k == 1)
        def _():
            for c in range(2, ROUNDS):
                basis_copy(c).wait()

        @pl.when(jnp.logical_and(k > 0, k < 5))
        def _():
            gram_blocks(2 + 6 * k, 6)

        @pl.when(k == 5)
        def _():
            gram_start()

        @pl.when(k == 6)
        def _():
            gram_middle()

        @pl.when(k == 7)
        def _():
            gram_last()

        wait_halo(k, par, ORDER[10:])
        unpack_yz(par)
        first_step((2, 3))
        wait_halo(k, par, ORDER[:10])
        unpack_x(par)
        first_step((0, 1, 4, 5))
        second_step(2 * k)
        wait_sent(k, par)
        got[pl.ds(2 * k, 2), g] = st[pl.ds(2 * k + 1, 2), g]
        return carry

    lax.fori_loop(0, ROUNDS, round_, 0)
    for o in (2, 1, 3):
        snap_copy(ROUNDS - 1, o).start()
    adj_copy = pltpu.make_async_copy(
        st.at[STEPS], joined.at[pl.ds(0, SPEC)], out_sem.at[0])
    adj_copy.start()
    for i in range(6):

        @pl.when(has(DIRS[i]))
        def _(i=i):
            coeff_copy(i).wait_send()

    flat = got.reshape(STEPS * 4 * ROWS, CZ)
    proj[...] = jnp.zeros_like(proj)
    unroll = 16

    def project(zq):
        def one(c, total):
            vals, blocks = [], []
            for u in range(unroll):
                at = c * unroll + u
                vals.append(flat[pl.ds(zq * ROWS + at, STEPS, stride=4 * ROWS), :])
                blocks.append(
                    bv[pl.ds(pl.multiple_of(at * 512 + zq * CZ, CZ), CZ), :])
            a = jnp.concatenate(vals, axis=1)
            hi = a.astype(BF16)
            lo = (a - hi.astype(F32)).astype(BF16)
            both = jnp.concatenate([hi, lo], axis=0)
            return total + jnp.dot(
                both, jnp.concatenate(blocks, axis=0), preferred_element_type=F32)

        proj[...] = lax.fori_loop(0, ROWS // unroll, one, proj[...])

    project(g)
    for o in (1, 3, 2):
        def snap_wait(k, carry, o=o):
            snap_copy(k, o).wait_recv()
            return carry

        lax.fori_loop(0, ROUNDS, snap_wait, 0)
        project(lax.rem(g + n_g - o, n_g))

    slot = lax.broadcasted_iota(jnp.int32, (SNAPS, MODES), 0)
    step_of = jnp.zeros((SNAPS, MODES), jnp.int32)
    for j in range(SNAPS):
        step_of = jnp.where(slot == j, plan[j], step_of)
    first = jnp.zeros((SNAPS, MODES), F32)
    for n in range(STEPS):
        row = proj[n:n + 1, :] + proj[STEPS + n:STEPS + n + 1, :]
        first = jnp.where(step_of == n, jnp.broadcast_to(row, first.shape), first)

    def all_sum(value):
        suma[ga] = value

        def a_copy(o):
            q, where = group_a(o)
            return pltpu.make_async_remote_copy(
                src_ref=suma.at[ga], dst_ref=suma.at[ga],
                send_sem=ss.at[0, o], recv_sem=sr.at[0, o],
                device_id=where, device_id_type=MESH)

        def b_copy(o):
            q, where = group_b(o)
            return pltpu.make_async_remote_copy(
                src_ref=sumb.at[x], dst_ref=sumb.at[x],
                send_sem=ss.at[1, o], recv_sem=sr.at[1, o],
                device_id=where, device_id_type=MESH)

        for o in range(1, n_g * n_y):
            a_copy(o).start()
        for o in range(1, n_g * n_y):
            gram_c(o).wait_recv()
        gm = gfull[...]
        g1 = gm.astype(BF16)
        left = gm - g1.astype(F32)
        g2 = left.astype(BF16)
        gsplit[0] = g1
        gsplit[1] = g2
        gsplit[2] = (left - g2.astype(F32)).astype(BF16)
        for o in range(1, n_g * n_y):
            a_copy(o).wait_recv()
        total = suma[0]
        for q in range(1, n_g * n_y):
            total = total + suma[q]
        sumb[x] = total
        for o in range(1, n_x):
            b_copy(o).start()
        for o in range(1, n_x):
            b_copy(o).wait_recv()
        total = sumb[0]
        for q in range(1, n_x):
            total = total + sumb[q]

        def finish():
            for o in range(1, n_g * n_y):
                a_copy(o).wait_send()
            for o in range(1, n_x):
                b_copy(o).wait_send()

        return total, finish

    total, finish = all_sum(first)
    low_first = total.astype(BF16)
    back = jnp.dot(low_first, gsplit[0], preferred_element_type=F32)
    back += jnp.dot(low_first, gsplit[1], preferred_element_type=F32)
    back += jnp.dot(low_first, gsplit[2], preferred_element_type=F32)
    result = total + (total - back)
    coeff_out[0:SNAPS, :] = result[:, 0:CZ]
    coeff_out[SNAPS:2 * SNAPS, :] = result[:, CZ:MODES]
    coeff_copy_out = pltpu.make_async_copy(coeff_out, joined.at[SPEC, 0], out_sem.at[1])
    coeff_copy_out.start()
    finish()
    for o in range(1, n_g * n_y):
        gram_a(o).wait_send()
        gram_c(o).wait_send()
    for o in range(1, n_x):
        gram_b(o).wait_send()

    def snap_sent(k, carry):
        for o in range(1, n_g):
            snap_copy(k, o).wait_send()
        return carry

    lax.fori_loop(0, ROUNDS, snap_sent, 0)
    adj_copy.wait()
    coeff_copy_out.wait()


def divide(joined, coeff_to, adj_to, field, coeff, sem):
    lead = pltpu.make_async_copy(joined.at[pl.ds(0, SPEC)], field, sem.at[0])
    tail = pltpu.make_async_copy(joined.at[SPEC, 0], coeff, sem.at[1])
    lead.start()
    tail.start()
    tail.wait()
    halves = [
        pltpu.make_async_copy(
            coeff.at[pl.ds(h * SNAPS, SNAPS), :], coeff_to.at[:, pl.ds(h * CZ, CZ)],
            sem.at[2 + h])
        for h in range(2)
    ]
    for half in halves:
        half.start()
    lead.wait()
    last = pltpu.make_async_copy(field, adj_to, sem.at[4])
    last.start()
    for half in halves:
        half.wait()
    last.wait()


def body(terminal, diffusion, velocity, material, rates, stoich, plan, basis):
    sm = pltpu.SMEM
    dma = pltpu.SemaphoreType.DMA
    v = pltpu.VMEM
    joined = pl.pallas_call(
        kernel,
        out_shape=jax.ShapeDtypeStruct((SPEC + 1, CX, CY, CZ), F32),
        in_specs=[pl.BlockSpec(memory_space=pl.ANY)] * 8,
        out_specs=pl.BlockSpec(memory_space=pl.ANY),
        scratch_shapes=[
            sm((SPEC,), F32),
            sm((MATS, 8), F32),
            sm((SPEC, 8), jnp.int32),
            sm((SNAPS,), jnp.int32),
            v((CX, CY, CZ), jnp.int32),
            v((CY, CZ), F32),
            dma((7,)),
            dma((2,)),
            v((BASIS_ROWS, MODES), BF16),
            v((STEPS + 1, SPEC, CX, CY, CZ), F32),
            v((2, CX, CY, CZ), F32),
            v((2, 2, SPEC, 2, CY, CZ), F32),
            v((2, 2, SPEC, CX // 2, 8, CZ), F32),
            v((2, 2, 8, CZ), F32),
            v((2, 2, SPEC, CX // 2, 8, CZ), F32),
            v((2, 6, 8, CZ), F32),
            v((2, 12, 8, CZ), F32),
            v((2, 2, 1, CY, CZ), F32),
            v((2, 2, CX, 8, CZ), F32),
            v((2, 2, CX, CY, CZ), F32),
            v((SPEC, 8, 24, 256), F32),
            v((SPEC, 6, 24, 256), F32),
            v((SPEC, 6, 24, 256), F32),
            v((6, 24, 256), F32),
            v((SPEC, 6, 24, 256), F32),
            v((SPEC, SPEC, 6, 24, 256), F32),
            v((MODES, MODES), F32),
            v((STEPS, 4, CX, CY, CZ), F32),
            v((2 * STEPS, MODES), F32),
            v((16, SNAPS, MODES), F32),
            v((8, SNAPS, MODES), F32),
            v((16, 16, MODES), F32),
            v((8, 16, MODES), F32),
            v((MODES, MODES), F32),
            v((3, MODES, MODES), BF16),
            dma((ROUNDS,)),
            dma((2, 18)),
            dma((2, 18)),
            dma((6,)),
            dma((6,)),
            dma((ROUNDS, 3)),
            dma((ROUNDS, 3)),
            dma((2, 16)),
            dma((2, 16)),
            dma((3, 16)),
            dma((3, 16)),
        ],
        compiler_params=pltpu.CompilerParams(
            collective_id=0, has_side_effects=True, vmem_limit_bytes=60 * 1024 * 1024
        ),
    )(
        terminal, diffusion, velocity, material, rates, stoich.T, plan,
        basis.reshape(BASIS_ROWS, MODES),
    )
    return pl.pallas_call(
        divide,
        out_shape=(
            jax.ShapeDtypeStruct((SNAPS, MODES), F32),
            jax.ShapeDtypeStruct((SPEC, CX, CY, CZ), F32),
        ),
        in_specs=[pl.BlockSpec(memory_space=pl.ANY)],
        out_specs=(pl.BlockSpec(memory_space=pl.ANY),) * 2,
        scratch_shapes=[v((SPEC, CX, CY, CZ), F32), v((CY, CZ), F32), dma((5,))],
        compiler_params=pltpu.CompilerParams(vmem_limit_bytes=60 * 1024 * 1024),
    )(joined)


def solution(mesh):
    return jax.shard_map(
        body,
        mesh=mesh,
        in_specs=(
            P(None, "gx", "gy", "grp"),
            P(),
            P("gx", "gy", "grp"),
            P("gx", "gy", "grp"),
            P(),
            P(),
            P(),
            P("grp", "gx", "gy", None, None),
        ),
        out_specs=(P(), P(None, "gx", "gy", "grp")),
        check_vma=False,
    )
```
